32 devices in a mesh: dp: 16 (over z, y, x), mp: 2 (over core).
Axes of the slice: x: 2, y: 2, z: 4, core: 2. Of those that a mesh axis runs over, the one named last changes fastest.
Arguments:
- pre_act: bfloat16 [8192, 16384], P('dp', 'mp'), may hold values from -8 to 8
- out_weight: bfloat16 [16384, 512], P('mp'), may hold values from -0.046875 to 0.046875
- out_grad: bfloat16 [8192, 512], P(('dp', 'mp')), may hold values from -2 to 2
Outputs:
- projected: bfloat16 [8192, 512], P(('dp', 'mp'))
- combined: float32 [16384, 512], P(('mp', 'dp'))
The draws below stay inside these ranges and needn't reach their ends.
All inputs are finite; a program needn't handle non-finite values.
Results may differ from the reference program's by a relative error of at most 0.0005.
Values may be sent and summed in bfloat16 or wider, within the bound.
A program may use at most 128 MiB of HBM per device.

```python
import math
import jax
import jax.numpy as jnp
from jax import lax

D = 512
FF = 16384
TOK_DEV = 512
TOKENS = 8192
N_DP = 16


def draw_pre_act(key, part):
    base = jax.random.normal(jax.random.fold_in(key, 11), (FF,), jnp.float32)
    noise = jax.random.normal(jax.random.fold_in(key, 12), (TOKENS, FF), jnp.float32)
    values = 0.6 * base[None, :] + noise
    return jnp.clip(values, -8.0, 8.0).astype(jnp.bfloat16)


def draw_out_grad(key, part):
    base = jax.random.normal(jax.random.fold_in(key, 21), (D,), jnp.float32)
    block_count = TOKENS // TOK_DEV
    block_scale = jnp.exp(jax.random.uniform(jax.random.fold_in(key, 23), (block_count,), jnp.float32, 0.0, math.log(10.0)))
    row_scale = jnp.exp(jax.random.uniform(jax.random.fold_in(key, 24), (TOKENS,), jnp.float32, -0.5, 0.5))
    scales = jnp.repeat(block_scale, TOK_DEV) * row_scale
    noise = jax.random.normal(jax.random.fold_in(key, 22), (TOKENS, D), jnp.float32)
    values = 0.06 * base[None, :] + noise
    return jnp.clip(0.025 * scales[:, None] * values, -2.0, 2.0).astype(jnp.bfloat16)


def levels(own_key, dims, split, low, top_value):
    gain, own = 1.0, jax.random.fold_in(own_key, 6)
    for axis_at, shards_of in split:
        draws = jnp.exp(jax.random.uniform(jax.random.fold_in(own, axis_at), (shards_of,), jnp.float32, low / len(split), top_value / len(split)))
        gain = gain * jnp.repeat(draws, dims[axis_at] // shards_of).reshape([-1 if axis == axis_at else 1 for axis in range(len(dims))])
    return gain


def scatter_about(key, shape, spread, reach, shards=(), held_as=jnp.bfloat16):
    entries = jax.random.normal(key, shape, jnp.float32) * spread
    if len(shards) > 0:
        entries = levels(key, shape, shards, -0.22, 0.18) * entries
    return jnp.clip(entries, min=-reach, max=reach).astype(held_as)


def setup_inputs(seed: int = 0) -> dict:
    key_of = jax.random.split(jax.random.key(seed), 4)
    return {
        "pre_act": draw_pre_act(jax.random.fold_in(key_of[3], 71), 0),
        "out_weight": scatter_about(key_of[1], (FF, D), FF ** -0.5, 0.046875, ((0, 2),)),
        "out_grad": draw_out_grad(jax.random.fold_in(key_of[3], 71), 0),
    }


epsilon = 1e-6


def pair(first, second):
    inner = jnp.sum(first * second)
    first_sq = jnp.sum(first * first)
    second_sq = jnp.sum(second * second)
    return (1.0 - inner / (2.0 * (first_sq + epsilon))) * first + (1.0 - inner / (2.0 * (second_sq + epsilon))) * second


def reference(pre_act, out_weight, out_grad):
    act = jnp.maximum(pre_act, jnp.zeros((), jnp.bfloat16))
    projected = jnp.dot(act, out_weight, preferred_element_type=jnp.float32).astype(jnp.bfloat16)

    def leaf(index):
        rows = act[index * TOK_DEV:(index + 1) * TOK_DEV]
        grads = out_grad[index * TOK_DEV:(index + 1) * TOK_DEV]
        return lax.dot_general(rows, grads, (((0,), (0,)), ((), ())), preferred_element_type=jnp.float32)

    def build(low, count):
        if count == 1:
            return leaf(low)
        half = count // 2
        return pair(build(low, half), build(low + half, half))

    combined = build(0, N_DP)
    return projected, combined
```

```python
import functools
import jax
import jax.numpy as jnp
from jax import lax
from jax.experimental import pallas as pl
from jax.experimental.pallas import tpu as pltpu
from jax.sharding import PartitionSpec as P

epsilon = 1e-06
MESH = pl.DeviceIdType.MESH


def from_partner(value, axis, apart):
    mask = 2**apart
    pairs = [(source, source ^ mask) for source in range(lax.axis_size(axis))]
    return lax.ppermute(value, axis, pairs)


def contract(left, right):
    return lax.dot_general(
        left, right, (((0,), (0,)), ((), ())), preferred_element_type=jnp.float32
    )


def split_rows(piece, block, which):
    width = piece.shape[1]
    blocks = piece.reshape(piece.shape[0] // (2 * block), 2, block, width)
    kept = lax.dynamic_index_in_dim(blocks, which, 1, False).reshape(-1, width)
    sent = lax.dynamic_index_in_dim(blocks, 1 - which, 1, False).reshape(-1, width)
    return (kept, sent)


def level_sums(partial_value, level):
    totals = lax.psum(partial_value, "mp")
    for inner_bit in range(level + 1):
        totals = totals + from_partner(totals, "dp", inner_bit)
    return totals


def merge_level(own, other, level, which):
    lower = which == 0
    own_sq = jnp.sum(own * own)
    other_sq = jnp.sum(other * other)
    partial_value = jnp.stack(
        [
            jnp.sum(own * other),
            jnp.where(lower, own_sq, other_sq),
            jnp.where(lower, other_sq, own_sq),
        ]
    )
    totals = level_sums(partial_value, level)
    first_coef = 1.0 - totals[0] / (2.0 * (totals[1] + epsilon))
    second_coef = 1.0 - totals[0] / (2.0 * (totals[2] + epsilon))
    own_coef = jnp.where(lower, first_coef, second_coef)
    other_coef = jnp.where(lower, second_coef, first_coef)
    return own_coef * own + other_coef * other


def halving(pre_act, out_weight, out_grad):
    act = jnp.maximum(pre_act, jnp.zeros((), jnp.bfloat16))
    tokens = act.shape[0]
    partial_out = jnp.dot(act, out_weight, preferred_element_type=jnp.float32)
    summed = lax.psum_scatter(partial_out, "mp", scatter_dimension=0, tiled=True)
    projected = summed.astype(jnp.bfloat16)
    grad_full = lax.all_gather(out_grad, "mp", axis=0, tiled=True)
    count = lax.axis_size("dp")
    levels = count.bit_length() - 1
    me = lax.axis_index("dp")
    block = act.shape[1] // count
    first_bit = me & 1
    groups = act.reshape(tokens, act.shape[1] // (2 * block), 2, block)
    kept_act = lax.dynamic_index_in_dim(groups, first_bit, 2, False).reshape(tokens, -1)
    sent_act = lax.dynamic_index_in_dim(groups, 1 - first_bit, 2, False).reshape(tokens, -1)
    packed = jnp.concatenate([sent_act, grad_full], axis=1)
    arrived = from_partner(packed, "dp", 0)
    half = sent_act.shape[1]
    own = contract(kept_act, grad_full)
    other = contract(arrived[:, :half], arrived[:, half:])
    piece = merge_level(own, other, 0, first_bit)
    for level in range(1, levels):
        which = me >> level & 1
        own, sent = split_rows(piece, block, which)
        other = from_partner(sent, "dp", level)
        piece = merge_level(own, other, level, which)
    return (projected, piece)


def row_of(values):
    parts = [jnp.sum(v, axis=0, keepdims=True) for v in values]
    parts += [jnp.zeros_like(parts[0])] * (8 - len(parts))
    table = jnp.concatenate(parts, axis=0)
    return line_of(table)


def line_of(table):
    totals = jnp.sum(table, axis=1, keepdims=True)
    lane = lax.broadcasted_iota(jnp.int32, table.shape, 1)
    row = lax.broadcasted_iota(jnp.int32, table.shape, 0)
    return jnp.sum(jnp.where(lane == row, totals, 0.0), axis=0, keepdims=True)


def lane_value(line, p):
    lane = lax.broadcasted_iota(jnp.int32, line.shape, 1)
    return jnp.sum(jnp.where(lane == p, line, 0.0), axis=1, keepdims=True)


def swap(value, axis, bit):
    size = value.shape[axis]
    at = lax.broadcasted_iota(jnp.int32, value.shape, axis)
    up = pltpu.roll(value, size - bit, axis)
    down = pltpu.roll(value, bit, axis)
    return jnp.where((at // bit) % 2 == 0, up, down)


def tree_coefs(line, group):
    rows = 2 * group
    lanes = line.shape[1]
    m = jnp.concatenate([pltpu.roll(jnp.broadcast_to(line, (8, lanes)), group * r, 1)[0:1] if r else line for r in range(rows)], axis=0)
    lane = lax.broadcasted_iota(jnp.int32, m.shape, 1)
    own = lax.broadcasted_iota(jnp.int32, m.shape, 0) % group
    coef = jnp.ones_like(m)
    for level in range(group.bit_length() - 1):
        bit = 2**level
        mate = jnp.where((own // bit) % 2 == 0, own + bit, own - bit)
        inner = jnp.sum(jnp.where(lane == mate, m, 0.0), axis=1, keepdims=True)
        square = jnp.sum(jnp.where(lane == own, m, 0.0), axis=1, keepdims=True)
        f = 1.0 - inner / (2.0 * (jnp.maximum(square, 0.0) + epsilon))
        f = jnp.broadcast_to(f, m.shape)
        coef = coef * f
        across = jnp.where(lane == own, f, 0.0)
        across = jnp.concatenate(
            [jnp.broadcast_to(jnp.sum(across[g * group:(g + 1) * group], axis=0, keepdims=True), (group, lanes)) for g in range(2)],
            axis=0,
        )
        m = m * f * across
        m = m + swap(m, 1, bit)
        m = m + swap(m, 0, bit)
    return coef


def kernel(
    n_dp, pre, w, og, proj, comb,
    acts, grads, leaf, node, arrived, xbuf, wbuf, acc, part_in, gsum, slots, slots3, coefs,
    act_send, act_recv, og_send, og_recv, mate_send, mate_recv, local_sem,
    fwd_sem, part_sem, slot_send, slot_recv, node_send, node_recv, slot3_send, slot3_recv,
):
    dp = lax.axis_index("dp")
    core = lax.axis_index("mp")
    group = n_dp // 2
    me = lax.rem(dp, group)
    z = dp // 4
    y = lax.rem(dp // 2, 2)
    x = lax.rem(dp, 2)
    high = z // 2
    zi = 2 * high + 1 - lax.rem(z, 2)
    tokens = pre.shape[0]
    block = pre.shape[1] // n_dp
    own_rows = og.shape[0]
    width = og.shape[1]
    mate = 1 - core
    edge_z, mid_z = 3 * high, 1 + high
    far_edge_z, far_mid_z = 3 - 3 * high, 2 - high
    edge = z == edge_z
    mid = z == mid_z

    def spot(at_z, m):
        dx = lax.rem(m, 2) if not isinstance(m, int) else m % 2
        dy = m // 2
        return at_z * 4 + (y + dy - 2 * dy * y) * 2 + x + dx - 2 * dx * x

    def turn(j):
        k = core * (ORDER[(j + 2) % 4] - ORDER[j]) + ORDER[j]
        return k

    barrier = pltpu.get_barrier_semaphore()
    for q in range(1, 2 * n_dp):
        other = lax.rem(dp * 2 + core + q, 2 * n_dp)
        pl.semaphore_signal(
            barrier, inc=1, device_id=(other // 2, lax.rem(other, 2)), device_id_type=MESH
        )

    def half(i, side):
        return grads.at[i, pl.ds(side * own_rows, own_rows)]

    og_local = pltpu.make_async_copy(og, half(dp, core), local_sem)
    og_local.start()

    def cols(b):
        return pl.ds(pl.multiple_of(b * block, block), block)

    def self_copy(b, slot):
        return pltpu.make_async_copy(pre.at[:, cols(b)], acts.at[slot], act_recv.at[slot])

    step_cols = xbuf.shape[2]
    steps = pre.shape[1] // step_cols

    def fetch(k, slot):
        here = pl.ds(pl.multiple_of(k * step_cols, step_cols), step_cols)
        return (
            pltpu.make_async_copy(pre.at[:, here], xbuf.at[slot], fwd_sem.at[slot, 0]),
            pltpu.make_async_copy(w.at[here, :], wbuf.at[slot], fwd_sem.at[slot, 1]),
        )

    for c in fetch(0, 0):
        c.start()
    acc[...] = jnp.zeros_like(acc)
    gsum[...] = jnp.zeros_like(gsum)

    def og_copy(n, i, to):
        return pltpu.make_async_remote_copy(
            src_ref=half(i, core), dst_ref=half(i, core), send_sem=og_send.at[n],
            recv_sem=og_recv.at[i], device_id=(to, core), device_id_type=MESH,
        )

    def mate_copy(i, side):
        return pltpu.make_async_remote_copy(
            src_ref=half(i, side), dst_ref=half(i, side), send_sem=mate_send.at[i],
            recv_sem=mate_recv.at[i], device_id=(dp, mate), device_id_type=MESH,
        )

    def og_arrival(i):
        og_copy(0, i, dp).wait_recv()
        mate_copy(i, core).start()

    def act_copy(kind, m):
        if kind < 2:
            to = spot(edge_z, m)
            b, slot = (to if kind == 0 else spot(far_edge_z, m)), me * 2 + kind
        else:
            to = spot(mid_z if kind == 2 else far_mid_z, m)
            b, slot = to, dp
        return pltpu.make_async_remote_copy(
            src_ref=pre.at[:, cols(b)], dst_ref=acts.at[slot],
            send_sem=act_send.at[kind * 4 + m], recv_sem=act_recv.at[slot],
            device_id=(to, core), device_id_type=MESH,
        )

    def plan(batch, where):
        return [(kind, turn(m - 4) if m > 3 else m) for kind, m in BATCHES[where][batch]]

    def send_acts(batch):
        for where, here in ((0, edge), (1, mid)):
            @pl.when(here)
            def _():
                for kind, m in plan(batch, where):
                    act_copy(kind, m).start()

    og_local.wait()
    pl.semaphore_wait(barrier, 2 * n_dp - 1)

    cross, along = 2 - core, 1 + core
    common = (
        ((z, 0, z, 1), (z, 0, z, 2), (z, 0, zi, 0)),
        ((z, cross, z, along), (z, 1, zi, 0), (z, 2, zi, 0)),
        ((z, 3, zi, 0),),
        (),
    )
    extra = (
        ((z, 0, far_mid_z, 0),),
        ((zi, 0, far_mid_z, 0), (far_mid_z, 0, z, 1), (far_mid_z, 0, z, 2)),
        ((z, 3, far_mid_z, 0), (far_edge_z, 0, z, 1), (far_edge_z, 0, z, 2)),
        ((far_edge_z, cross, z, along),),
    )
    landed = (
        ((), ()),
        (((z, 1), (z, 2), (zi, 0)), ((far_mid_z, 0),)),
        (((z, 3), (zi, 1), (zi, 2)), ((far_edge_z, 0), (far_mid_z, 1), (far_mid_z, 2))),
        (((zi, 3),), ((far_mid_z, 3), (far_edge_z, 1), (far_edge_z, 2))),
        ((), ((far_edge_z, 3),)),
    )

    def og_wave(k, moves):
        base = sum(len(c) for c in moves[:k])
        base += sum(len(c) for c in common) if moves is extra else 0
        return [og_copy(base + n, spot(a, m), spot(b, r)) for n, (a, m, b, r) in enumerate(moves[k])]

    def wave(k):
        for i in landed[k][0]:
            og_arrival(spot(*i))

        @pl.when(mid)
        def _():
            for i in landed[k][1]:
                og_arrival(spot(*i))

        if k < len(common):
            for c in og_wave(k, common):
                c.start()

            @pl.when(mid)
            def _():
                for c in og_wave(k, extra):
                    c.start()

            send_acts(k)

    wave(0)
    mate_copy(dp, core).start()

    @pl.when(edge)
    def _():
        self_copy(dp, me * 2).start()
        self_copy(spot(far_edge_z, 0), me * 2 + 1).start()

    @pl.when(mid)
    def _():
        self_copy(dp, dp).start()

    def forward(k, carry):
        slot = lax.rem(k, 2)

        @pl.when(k + 1 < steps)
        def _():
            for c in fetch(k + 1, 1 - slot):
                c.start()

        for c in fetch(k, slot):
            c.wait()
        v = jnp.maximum(xbuf[slot], jnp.zeros((), jnp.bfloat16))
        acc[...] += jnp.dot(v, wbuf[slot], preferred_element_type=jnp.float32)
        return carry

    lax.fori_loop(0, steps, forward, 0)
    part = pltpu.make_async_remote_copy(
        src_ref=acc.at[pl.ds(mate * own_rows, own_rows)], dst_ref=part_in,
        send_sem=part_sem.at[0], recv_sem=part_sem.at[1],
        device_id=(dp, mate), device_id_type=MESH,
    )
    part.start()
    wave(1)
    part.wait_recv()
    proj[...] = (acc[pl.ds(core * own_rows, own_rows), :] + part_in[...]).astype(proj.dtype)
    wave(2)
    wave(3)
    wave(4)

    def settle(i):
        mate_copy(i, mate).wait_recv()

    def leaf_grad(i, slot, own):
        if own:
            self_copy(0, slot).wait()
        else:
            pltpu.make_async_remote_copy(
                src_ref=pre.at[:, cols(0)], dst_ref=acts.at[slot], send_sem=act_send.at[0],
                recv_sem=act_recv.at[slot], device_id=(dp, mate), device_id_type=MESH,
            ).wait_recv()
        a = jnp.maximum(acts[slot], jnp.zeros((), jnp.bfloat16))
        leaf[slot] = contract(a, grads[i])

    def gram(new, others):
        i, slot = new
        seen = others + [new]

        def strip(t, carry):
            rows = pl.ds(pl.multiple_of(t * 8, 8), 8)
            for c in range(width // 128):
                lanes = slice(c * 128, (c + 1) * 128)
                v = leaf[slot, rows, lanes]
                carry = tuple(s + v * leaf[o, rows, lanes] for s, (_, o) in zip(carry, seen[:-1])) + (carry[-1] + v * v,)
            return carry

        zero = jnp.zeros((8, 128), jnp.float32)
        sums = lax.fori_loop(0, block // 8, strip, (zero,) * len(seen))
        for s, (j, _) in zip(sums, seen):
            line = jnp.sum(s, axis=0, keepdims=True)
            for p, q in ((i, j), (j, i))[: 1 if j is i else 2]:
                at = pl.ds(lax.rem(2 * group - p, 2 * group) * group + lax.rem(q, group), 1)
                gsum[at, :] += line

    @pl.when(edge)
    def _():
        def both(h, carry):
            done = []
            for n, (at_z, m) in enumerate([(z, 0), (z, 3), (z, 2), (z, 1)] + [(zi, turn(j)) for j in range(4)]):
                i = spot(at_z, m)

                @pl.when(h == 0)
                def _():
                    settle(i)

                slot = lax.rem(i, group) * 2 + h
                leaf_grad(i, slot, n == 0)
                gram((i, slot), done)
                done = done + [(i, slot)]
            return carry

        lax.fori_loop(0, 2, both, 0)

    @pl.when(mid)
    def _():
        near, away = [], []

        def take(i, seen):
            settle(i)
            leaf_grad(i, i, i is home)
            gram((i, i), seen)
            seen.append((i, i))

        home = spot(z, 0)
        take(home, near)
        for m in (3, 2, 1):
            take(spot(z, m), near)
        for j in range(4):
            take(spot(far_edge_z, turn(j)), away)
        for j in range(4):
            take(spot(far_mid_z, turn(j)), away)
            take(spot(zi, turn(j)), near)

    def gather(buf, send, recv, line):
        mine = dp * 2 + core
        buf[mine] = line

        def copy(q, other, at):
            return pltpu.make_async_remote_copy(
                src_ref=buf.at[at], dst_ref=buf.at[at], send_sem=send.at[q], recv_sem=recv.at[at],
                device_id=(other // 2, lax.rem(other, 2)), device_id_type=MESH,
            )

        def go(q, carry):
            copy(q, lax.rem(mine + q, 2 * n_dp), mine).start()
            return carry

        def take(q, carry):
            other = lax.rem(mine + q, 2 * n_dp)
            copy(q, other, other).wait_recv()
            return carry

        def left(q, carry):
            copy(q, lax.rem(mine + q, 2 * n_dp), mine).wait_send()
            return carry

        def finish():
            lax.fori_loop(1, 2 * n_dp, take, 0)
            total = buf[0]
            for k in range(1, 2 * n_dp):
                total = total + buf[k]
            return total

        lax.fori_loop(1, 2 * n_dp, go, 0)
        return finish, lambda: lax.fori_loop(1, 2 * n_dp, left, 0)

    finish, sent = gather(slots, slot_send, slot_recv, line_of(gsum[...]))
    coefs[...] = tree_coefs(finish(), group)

    def weights(first):
        return [jnp.broadcast_to(coefs[pl.ds(first + k, 1), :], (8, 128)) for k in range(group)]

    pieces = node_send.shape[0]
    tall = block // pieces

    def mix(weight, places, rows, lanes):
        total = weight[0] * leaf[places[0], rows, lanes]
        for k in range(1, group):
            total = total + weight[k] * leaf[places[k], rows, lanes]
        return total

    zero = jnp.zeros((8, 128), jnp.float32)
    far = spot(far_edge_z, 0)

    def node_copy(k):
        rows = pl.ds(k * tall, tall)
        return pltpu.make_async_remote_copy(
            src_ref=node.at[1, rows], dst_ref=arrived.at[rows],
            send_sem=node_send.at[k], recv_sem=node_recv.at[k],
            device_id=(far, core), device_id_type=MESH,
        )

    sums3 = slots3.at[dp * 2 + core]
    up = high.astype(jnp.float32)

    @pl.when(edge)
    def _():
        weight = weights(high * group)

        def build(h, first, count, q):
            def strip(t, q):
                rows = pl.ds(pl.multiple_of(first + t * 8, 8), 8)
                for c in range(width // 128):
                    lanes = slice(c * 128, (c + 1) * 128)
                    total = mix(weight, [2 * k + h for k in range(group)], rows, lanes)
                    node[h, rows, lanes] = total
                    q = q + total * total
                return q
            return lax.fori_loop(0, count // 8, strip, q)

        q = zero
        for k in range(pieces):
            q = build(1, k * tall, tall, q)
            node_copy(k).start()
        q = build(0, 0, block, q)
        s = zero
        for k in range(pieces):
            node_copy(k).wait_recv()

            def inner(t, s):
                rows = pl.ds(pl.multiple_of(k * tall + t * 8, 8), 8)
                for c in range(width // 128):
                    lanes = slice(c * 128, (c + 1) * 128)
                    s = s + node[0, rows, lanes] * arrived[rows, lanes]
                return s

            s = lax.fori_loop(0, tall // 8, inner, s)
        sums3[...] = row_of([s, (1.0 - up) * q, up * q])

    @pl.when(mid)
    def _():
        low, top = weights(0), weights(group)

        def strip(t, carry):
            rows = pl.ds(pl.multiple_of(t * 8, 8), 8)
            s, q, r = carry
            for c in range(width // 128):
                lanes = slice(c * 128, (c + 1) * 128)
                a = mix(low, range(group), rows, lanes)
                b = mix(top, range(group, 2 * group), rows, lanes)
                node[0, rows, lanes] = a
                node[1, rows, lanes] = b
                s, q, r = s + a * b, q + a * a, r + b * b
            return s, q, r

        s, q, r = lax.fori_loop(0, block // 8, strip, (zero,) * 3)
        sums3[...] = row_of([s, q, r])

    finish3, sent3 = gather(slots3, slot3_send, slot3_recv, slots3[dp * 2 + core])
    line = finish3()
    s = lane_value(line, 0)
    low = jnp.broadcast_to(1.0 - s / (2.0 * (lane_value(line, 1) + epsilon)), (8, width))
    top = jnp.broadcast_to(1.0 - s / (2.0 * (lane_value(line, 2) + epsilon)), (8, width))

    def last(first, second, other):
        def strip(t, carry):
            rows = pl.ds(pl.multiple_of(t * 8, 8), 8)
            comb[rows, :] = first * node[0, rows, :] + second * other[rows, :]
            return carry
        lax.fori_loop(0, block // 8, strip, 0)

    @pl.when(edge)
    def _():
        last((1.0 - up) * low + up * top, up * low + (1.0 - up) * top, arrived)

    @pl.when(mid)
    def _():
        last(low, top, node.at[1])

    mate_copy(dp, core).wait_send()
    for k in range(len(landed)):
        for i in landed[k][0]:
            mate_copy(spot(*i), core).wait_send()
        if k < len(common):
            for c in og_wave(k, common):
                c.wait_send()
    part.wait_send()

    @pl.when(mid)
    def _():
        for k in range(len(landed)):
            for i in landed[k][1]:
                mate_copy(spot(*i), core).wait_send()
            if k < len(common):
                for c in og_wave(k, extra):
                    c.wait_send()
                for kind, m in plan(k, 1):
                    act_copy(kind, m).wait_send()

    @pl.when(edge)
    def _():
        for k in range(len(common)):
            for kind, m in plan(k, 0):
                act_copy(kind, m).wait_send()
        for k in range(pieces):
            node_copy(k).wait_send()

    sent()
    sent3()


ORDER = (3, 1, 0, 2)
BATCHES = (
    (
        ((3, 4), (0, 3), (0, 2)),
        ((3, 5), (0, 1)),
        ((3, 6), (1, 3), (1, 2)),
        ((3, 7), (1, 1), (2, 4), (2, 5), (2, 6), (2, 7)),
    ),
    (
        ((3, 4), (0, 4), (2, 3), (2, 2)),
        ((3, 5), (0, 5), (2, 1)),
        ((3, 6), (0, 6)),
        ((3, 7), (0, 7), (1, 4), (1, 5), (1, 6), (1, 7)),
    ),
)


def exchange(n_dp, pre_act, out_weight, out_grad):
    tokens, hidden = pre_act.shape
    block = hidden // n_dp
    width = out_grad.shape[1]
    own_rows = out_grad.shape[0]
    step_cols = hidden // 8
    pieces = 4
    dma = pltpu.SemaphoreType.DMA
    hbm = pl.BlockSpec(memory_space=pl.ANY)
    vmem = pl.BlockSpec(memory_space=pltpu.VMEM)
    return pl.pallas_call(
        functools.partial(kernel, n_dp),
        out_shape=(
            jax.ShapeDtypeStruct((own_rows, width), jnp.bfloat16),
            jax.ShapeDtypeStruct((block, width), jnp.float32),
        ),
        in_specs=[hbm, hbm, hbm],
        out_specs=(vmem, vmem),
        scratch_shapes=[
            pltpu.VMEM((n_dp, tokens, block), jnp.bfloat16),
            pltpu.VMEM((n_dp, tokens, width), jnp.bfloat16),
            pltpu.VMEM((n_dp, block, width), jnp.float32),
            pltpu.VMEM((2, block, width), jnp.float32),
            pltpu.VMEM((block, width), jnp.float32),
            pltpu.VMEM((2, tokens, step_cols), jnp.bfloat16),
            pltpu.VMEM((2, step_cols, width), jnp.bfloat16),
            pltpu.VMEM((tokens, width), jnp.float32),
            pltpu.VMEM((own_rows, width), jnp.float32),
            pltpu.VMEM((128, 128), jnp.float32),
            pltpu.VMEM((2 * n_dp, 1, 128), jnp.float32),
            pltpu.VMEM((2 * n_dp, 1, 128), jnp.float32),
            pltpu.VMEM((n_dp, 128), jnp.float32),
            dma((16,)), dma((n_dp,)), dma((16,)), dma((n_dp,)), dma((n_dp,)), dma((n_dp,)), dma,
            dma((2, 2)), dma((2,)), dma((2 * n_dp,)), dma((2 * n_dp,)),
            dma((pieces,)), dma((pieces,)), dma((2 * n_dp,)), dma((2 * n_dp,)),
        ],
        compiler_params=pltpu.CompilerParams(
            collective_id=0, has_side_effects=True, vmem_limit_bytes=60 * 2**20
        ),
    )(pre_act, out_weight, out_grad)


def local(pre_act, out_weight, out_grad):
    n_dp = lax.axis_size("dp")
    block = pre_act.shape[1] // n_dp
    rows = out_grad.shape[0]
    if lax.axis_size("mp") == 2 and n_dp == 4 * len(ORDER) and block % 128 == 0 and rows % 16 == 0:
        return exchange(n_dp, pre_act, out_weight, out_grad)
    return halving(pre_act, out_weight, out_grad)


def solution(mesh):
    placed = (P("dp", "mp"), P("mp", None), P(("dp", "mp"), None))
    return jax.shard_map(
        local,
        mesh=mesh,
        in_specs=placed,
        out_specs=(P(("dp", "mp"), None), P(("mp", "dp"), None)),
        check_vma=False,
    )
```

```python
import functools
import jax
import jax.numpy as jnp
from jax import lax
from jax.experimental import pallas as pl
from jax.experimental.pallas import tpu as pltpu
from jax.sharding import PartitionSpec as P

epsilon = 1e-06
MESH = pl.DeviceIdType.MESH


def from_partner(value, axis, apart):
    mask = 2**apart
    pairs = [(source, source ^ mask) for source in range(lax.axis_size(axis))]
    return lax.ppermute(value, axis, pairs)


def contract(left, right):
    return lax.dot_general(
        left, right, (((0,), (0,)), ((), ())), preferred_element_type=jnp.float32
    )


def split_rows(piece, block, which):
    width = piece.shape[1]
    blocks = piece.reshape(piece.shape[0] // (2 * block), 2, block, width)
    kept = lax.dynamic_index_in_dim(blocks, which, 1, False).reshape(-1, width)
    sent = lax.dynamic_index_in_dim(blocks, 1 - which, 1, False).reshape(-1, width)
    return (kept, sent)


def level_sums(partial_value, level):
    totals = lax.psum(partial_value, "mp")
    for inner_bit in range(level + 1):
        totals = totals + from_partner(totals, "dp", inner_bit)
    return totals


def merge_level(own, other, level, which):
    lower = which == 0
    own_sq = jnp.sum(own * own)
    other_sq = jnp.sum(other * other)
    partial_value = jnp.stack(
        [
            jnp.sum(own * other),
            jnp.where(lower, own_sq, other_sq),
            jnp.where(lower, other_sq, own_sq),
        ]
    )
    totals = level_sums(partial_value, level)
    first_coef = 1.0 - totals[0] / (2.0 * (totals[1] + epsilon))
    second_coef = 1.0 - totals[0] / (2.0 * (totals[2] + epsilon))
    own_coef = jnp.where(lower, first_coef, second_coef)
    other_coef = jnp.where(lower, second_coef, first_coef)
    return own_coef * own + other_coef * other


def halving(pre_act, out_weight, out_grad):
    act = jnp.maximum(pre_act, jnp.zeros((), jnp.bfloat16))
    tokens = act.shape[0]
    partial_out = jnp.dot(act, out_weight, preferred_element_type=jnp.float32)
    summed = lax.psum_scatter(partial_out, "mp", scatter_dimension=0, tiled=True)
    projected = summed.astype(jnp.bfloat16)
    grad_full = lax.all_gather(out_grad, "mp", axis=0, tiled=True)
    count = lax.axis_size("dp")
    levels = count.bit_length() - 1
    me = lax.axis_index("dp")
    block = act.shape[1] // count
    first_bit = me & 1
    groups = act.reshape(tokens, act.shape[1] // (2 * block), 2, block)
    kept_act = lax.dynamic_index_in_dim(groups, first_bit, 2, False).reshape(tokens, -1)
    sent_act = lax.dynamic_index_in_dim(groups, 1 - first_bit, 2, False).reshape(tokens, -1)
    packed = jnp.concatenate([sent_act, grad_full], axis=1)
    arrived = from_partner(packed, "dp", 0)
    half = sent_act.shape[1]
    own = contract(kept_act, grad_full)
    other = contract(arrived[:, :half], arrived[:, half:])
    piece = merge_level(own, other, 0, first_bit)
    for level in range(1, levels):
        which = me >> level & 1
        own, sent = split_rows(piece, block, which)
        other = from_partner(sent, "dp", level)
        piece = merge_level(own, other, level, which)
    return (projected, piece)


def row_of(values):
    parts = [jnp.sum(v, axis=0, keepdims=True) for v in values]
    parts += [jnp.zeros_like(parts[0])] * (8 - len(parts))
    table = jnp.concatenate(parts, axis=0)
    return line_of(table)


def line_of(table):
    totals = jnp.sum(table, axis=1, keepdims=True)
    lane = lax.broadcasted_iota(jnp.int32, table.shape, 1)
    row = lax.broadcasted_iota(jnp.int32, table.shape, 0)
    return jnp.sum(jnp.where(lane == row, totals, 0.0), axis=0, keepdims=True)


def lane_value(line, p):
    lane = lax.broadcasted_iota(jnp.int32, line.shape, 1)
    return jnp.sum(jnp.where(lane == p, line, 0.0), axis=1, keepdims=True)


def swap(value, axis, bit):
    size = value.shape[axis]
    at = lax.broadcasted_iota(jnp.int32, value.shape, axis)
    up = pltpu.roll(value, size - bit, axis)
    down = pltpu.roll(value, bit, axis)
    return jnp.where((at // bit) % 2 == 0, up, down)


def tree_coefs(line, group):
    rows = 2 * group
    lanes = line.shape[1]
    m = jnp.concatenate([pltpu.roll(jnp.broadcast_to(line, (8, lanes)), group * r, 1)[0:1] if r else line for r in range(rows)], axis=0)
    lane = lax.broadcasted_iota(jnp.int32, m.shape, 1)
    own = lax.broadcasted_iota(jnp.int32, m.shape, 0) % group
    coef = jnp.ones_like(m)
    for level in range(group.bit_length() - 1):
        bit = 2**level
        mate = jnp.where((own // bit) % 2 == 0, own + bit, own - bit)
        inner = jnp.sum(jnp.where(lane == mate, m, 0.0), axis=1, keepdims=True)
        square = jnp.sum(jnp.where(lane == own, m, 0.0), axis=1, keepdims=True)
        f = 1.0 - inner / (2.0 * (jnp.maximum(square, 0.0) + epsilon))
        f = jnp.broadcast_to(f, m.shape)
        coef = coef * f
        across = jnp.where(lane == own, f, 0.0)
        across = jnp.concatenate(
            [jnp.broadcast_to(jnp.sum(across[g * group:(g + 1) * group], axis=0, keepdims=True), (group, lanes)) for g in range(2)],
            axis=0,
        )
        m = m * f * across
        m = m + swap(m, 1, bit)
        m = m + swap(m, 0, bit)
    return coef


def kernel(
    n_dp, pre, w, og, proj, comb,
    acts, grads, leaf, node, arrived, xbuf, wbuf, acc, part_in, gsum, slots, slots3, coefs,
    act_send, act_recv, og_send, og_recv, mate_send, mate_recv, local_sem,
    fwd_sem, part_sem, slot_send, slot_recv, node_send, node_recv, slot3_send, slot3_recv,
):
    dp = lax.axis_index("dp")
    core = lax.axis_index("mp")
    group = n_dp // 2
    me = lax.rem(dp, group)
    z = dp // 4
    y = lax.rem(dp // 2, 2)
    x = lax.rem(dp, 2)
    high = z // 2
    zi = 2 * high + 1 - lax.rem(z, 2)
    tokens = pre.shape[0]
    block = pre.shape[1] // n_dp
    own_rows = og.shape[0]
    width = og.shape[1]
    mate = 1 - core
    edge_z, mid_z = 3 * high, 1 + high
    far_edge_z, far_mid_z = 3 - 3 * high, 2 - high
    edge = z == edge_z
    mid = z == mid_z

    def spot(at_z, m):
        dx = lax.rem(m, 2) if not isinstance(m, int) else m % 2
        dy = m // 2
        return at_z * 4 + (y + dy - 2 * dy * y) * 2 + x + dx - 2 * dx * x

    def turn(j):
        k = core * (ORDER[(j + 2) % 4] - ORDER[j]) + ORDER[j]
        return k

    barrier = pltpu.get_barrier_semaphore()
    for q in range(1, 2 * n_dp):
        other = lax.rem(dp * 2 + core + q, 2 * n_dp)
        pl.semaphore_signal(
            barrier, inc=1, device_id=(other // 2, lax.rem(other, 2)), device_id_type=MESH
        )

    def half(i, side):
        return grads.at[i, pl.ds(side * own_rows, own_rows)]

    og_local = pltpu.make_async_copy(og, half(dp, core), local_sem)
    og_local.start()

    def cols(b):
        return pl.ds(pl.multiple_of(b * block, block), block)

    def self_copy(b, slot):
        return pltpu.make_async_copy(pre.at[:, cols(b)], acts.at[slot], act_recv.at[slot])

    step_cols = xbuf.shape[2]
    steps = pre.shape[1] // step_cols

    def fetch(k, slot):
        here = pl.ds(pl.multiple_of(k * step_cols, step_cols), step_cols)
        return (
            pltpu.make_async_copy(pre.at[:, here], xbuf.at[slot], fwd_sem.at[slot, 0]),
            pltpu.make_async_copy(w.at[here, :], wbuf.at[slot], fwd_sem.at[slot, 1]),
        )

    for c in fetch(0, 0):
        c.start()
    acc[...] = jnp.zeros_like(acc)
    gsum[...] = jnp.zeros_like(gsum)

    def og_copy(n, i, to):
        return pltpu.make_async_remote_copy(
            src_ref=half(i, core), dst_ref=half(i, core), send_sem=og_send.at[n],
            recv_sem=og_recv.at[i], device_id=(to, core), device_id_type=MESH,
        )

    def mate_copy(i, side):
        return pltpu.make_async_remote_copy(
            src_ref=half(i, side), dst_ref=half(i, side), send_sem=mate_send.at[i],
            recv_sem=mate_recv.at[i], device_id=(dp, mate), device_id_type=MESH,
        )

    def og_arrival(i):
        og_copy(0, i, dp).wait_recv()
        mate_copy(i, core).start()

    def act_copy(kind, m):
        if kind < 2:
            to = spot(edge_z, m)
            b, slot = (to if kind == 0 else spot(far_edge_z, m)), me * 2 + kind
        else:
            to = spot(mid_z if kind == 2 else far_mid_z, m)
            b, slot = to, dp
        return pltpu.make_async_remote_copy(
            src_ref=pre.at[:, cols(b)], dst_ref=acts.at[slot],
            send_sem=act_send.at[kind * 4 + m], recv_sem=act_recv.at[slot],
            device_id=(to, core), device_id_type=MESH,
        )

    def plan(batch, where):
        return [(kind, turn(m - 4) if m > 3 else m) for kind, m in BATCHES[where][batch]]

    def send_acts(batch):
        for where, here in ((0, edge), (1, mid)):
            @pl.when(here)
            def _():
                for kind, m in plan(batch, where):
                    act_copy(kind, m).start()

    og_local.wait()
    pl.semaphore_wait(barrier, 2 * n_dp - 1)

    common = (
        ((z, 0, far_mid_z, 0), (z, 0, zi, 0), (z, 0, z, 3), (z, 0, z, 1), (z, 0, z, 2)),
        ((z, 1, zi, 0), (z, 2, zi, 0), (z, 3, zi, 0)),
    )
    extra = (
        (),
        (
            (z, 1, far_mid_z, 0), (z, 2, far_mid_z, 0), (z, 3, far_mid_z, 0),
            (far_edge_z, 0, z, 3), (far_edge_z, 0, z, 1), (far_edge_z, 0, z, 2),
        ),
    )
    landed = (
        ((), ()),
        (((z, 1), (z, 2), (z, 3), (zi, 0)), ((far_mid_z, 0), (far_edge_z, 0))),
        (
            ((zi, 1), (zi, 2), (zi, 3)),
            tuple((far_mid_z, m) for m in (1, 2, 3)) + tuple((far_edge_z, m) for m in (1, 2, 3)),
        ),
    )

    def og_wave(k, moves):
        base = sum(len(c) for c in moves[:k])
        base += sum(len(c) for c in common) if moves is extra else 0
        return [og_copy(base + n, spot(a, m), spot(b, r)) for n, (a, m, b, r) in enumerate(moves[k])]

    def wave(k):
        for i in landed[k][0]:
            og_arrival(spot(*i))

        @pl.when(mid)
        def _():
            for i in landed[k][1]:
                og_arrival(spot(*i))

        if k < len(common):
            for c in og_wave(k, common):
                c.start()

            @pl.when(mid)
            def _():
                for c in og_wave(k, extra):
                    c.start()

            send_acts(k)

    wave(0)
    mate_copy(dp, core).start()

    @pl.when(edge)
    def _():
        self_copy(dp, me * 2).start()
        self_copy(spot(far_edge_z, 0), me * 2 + 1).start()

    @pl.when(mid)
    def _():
        self_copy(dp, dp).start()

    def forward(k, carry):
        slot = lax.rem(k, 2)

        @pl.when(k + 1 < steps)
        def _():
            for c in fetch(k + 1, 1 - slot):
                c.start()

        for c in fetch(k, slot):
            c.wait()
        v = jnp.maximum(xbuf[slot], jnp.zeros((), jnp.bfloat16))
        acc[...] += jnp.dot(v, wbuf[slot], preferred_element_type=jnp.float32)
        return carry

    lax.fori_loop(0, steps, forward, 0)
    part = pltpu.make_async_remote_copy(
        src_ref=acc.at[pl.ds(mate * own_rows, own_rows)], dst_ref=part_in,
        send_sem=part_sem.at[0], recv_sem=part_sem.at[1],
        device_id=(dp, mate), device_id_type=MESH,
    )
    part.start()
    wave(1)
    part.wait_recv()
    proj[...] = (acc[pl.ds(core * own_rows, own_rows), :] + part_in[...]).astype(proj.dtype)
    wave(2)

    def settle(i):
        mate_copy(i, mate).wait_recv()

    def leaf_grad(i, slot, own):
        if own:
            self_copy(0, slot).wait()
        else:
            pltpu.make_async_remote_copy(
                src_ref=pre.at[:, cols(0)], dst_ref=acts.at[slot], send_sem=act_send.at[0],
                recv_sem=act_recv.at[slot], device_id=(dp, mate), device_id_type=MESH,
            ).wait_recv()
        a = jnp.maximum(acts[slot], jnp.zeros((), jnp.bfloat16))
        leaf[slot] = contract(a, grads[i])

    def gram(new, others):
        i, slot = new
        seen = others + [new]

        def strip(t, carry):
            rows = pl.ds(pl.multiple_of(t * 8, 8), 8)
            for c in range(width // 128):
                lanes = slice(c * 128, (c + 1) * 128)
                v = leaf[slot, rows, lanes]
                carry = tuple(s + v * leaf[o, rows, lanes] for s, (_, o) in zip(carry, seen[:-1])) + (carry[-1] + v * v,)
            return carry

        zero = jnp.zeros((8, 128), jnp.float32)
        sums = lax.fori_loop(0, block // 8, strip, (zero,) * len(seen))
        for s, (j, _) in zip(sums, seen):
            line = jnp.sum(s, axis=0, keepdims=True)
            for p, q in ((i, j), (j, i))[: 1 if j is i else 2]:
                at = pl.ds(lax.rem(2 * group - p, 2 * group) * group + lax.rem(q, group), 1)
                gsum[at, :] += line

    @pl.when(edge)
    def _():
        def both(h, carry):
            done = []
            for n, (at_z, m) in enumerate([(z, 0), (z, 3), (z, 2), (z, 1)] + [(zi, turn(j)) for j in range(4)]):
                i = spot(at_z, m)

                @pl.when(h == 0)
                def _():
                    settle(i)

                slot = lax.rem(i, group) * 2 + h
                leaf_grad(i, slot, n == 0)
                gram((i, slot), done)
                done = done + [(i, slot)]
            return carry

        lax.fori_loop(0, 2, both, 0)

    @pl.when(mid)
    def _():
        near, away = [], []

        def take(i, seen):
            settle(i)
            leaf_grad(i, i, i is home)
            gram((i, i), seen)
            seen.append((i, i))

        home = spot(z, 0)
        take(home, near)
        for m in (3, 2, 1):
            take(spot(z, m), near)
        for j in range(4):
            take(spot(far_edge_z, turn(j)), away)
        for j in range(4):
            take(spot(far_mid_z, turn(j)), away)
            take(spot(zi, turn(j)), near)

    def gather(buf, send, recv, line):
        mine = dp * 2 + core
        buf[mine] = line

        def copy(q, other, at):
            return pltpu.make_async_remote_copy(
                src_ref=buf.at[at], dst_ref=buf.at[at], send_sem=send.at[q], recv_sem=recv.at[at],
                device_id=(other // 2, lax.rem(other, 2)), device_id_type=MESH,
            )

        def go(q, carry):
            copy(q, lax.rem(mine + q, 2 * n_dp), mine).start()
            return carry

        def take(q, carry):
            other = lax.rem(mine + q, 2 * n_dp)
            copy(q, other, other).wait_recv()
            return carry

        def left(q, carry):
            copy(q, lax.rem(mine + q, 2 * n_dp), mine).wait_send()
            return carry

        def finish():
            lax.fori_loop(1, 2 * n_dp, take, 0)
            total = buf[0]
            for k in range(1, 2 * n_dp):
                total = total + buf[k]
            return total

        lax.fori_loop(1, 2 * n_dp, go, 0)
        return finish, lambda: lax.fori_loop(1, 2 * n_dp, left, 0)

    finish, sent = gather(slots, slot_send, slot_recv, line_of(gsum[...]))
    coefs[...] = tree_coefs(finish(), group)

    def weights(first):
        return [jnp.broadcast_to(coefs[pl.ds(first + k, 1), :], (8, 128)) for k in range(group)]

    pieces = node_send.shape[0]
    tall = block // pieces

    def mix(weight, places, rows, lanes):
        total = weight[0] * leaf[places[0], rows, lanes]
        for k in range(1, group):
            total = total + weight[k] * leaf[places[k], rows, lanes]
        return total

    zero = jnp.zeros((8, 128), jnp.float32)
    far = spot(far_edge_z, 0)

    def node_copy(k):
        rows = pl.ds(k * tall, tall)
        return pltpu.make_async_remote_copy(
            src_ref=node.at[1, rows], dst_ref=arrived.at[rows],
            send_sem=node_send.at[k], recv_sem=node_recv.at[k],
            device_id=(far, core), device_id_type=MESH,
        )

    sums3 = slots3.at[dp * 2 + core]
    up = high.astype(jnp.float32)

    @pl.when(edge)
    def _():
        weight = weights(high * group)

        def build(h, first, count, q):
            def strip(t, q):
                rows = pl.ds(pl.multiple_of(first + t * 8, 8), 8)
                for c in range(width // 128):
                    lanes = slice(c * 128, (c + 1) * 128)
                    total = mix(weight, [2 * k + h for k in range(group)], rows, lanes)
                    node[h, rows, lanes] = total
                    q = q + total * total
                return q
            return lax.fori_loop(0, count // 8, strip, q)

        q = zero
        for k in range(pieces):
            q = build(1, k * tall, tall, q)
            node_copy(k).start()
        q = build(0, 0, block, q)
        s = zero
        for k in range(pieces):
            node_copy(k).wait_recv()

            def inner(t, s):
                rows = pl.ds(pl.multiple_of(k * tall + t * 8, 8), 8)
                for c in range(width // 128):
                    lanes = slice(c * 128, (c + 1) * 128)
                    s = s + node[0, rows, lanes] * arrived[rows, lanes]
                return s

            s = lax.fori_loop(0, tall // 8, inner, s)
        sums3[...] = row_of([s, (1.0 - up) * q, up * q])

    @pl.when(mid)
    def _():
        low, top = weights(0), weights(group)

        def strip(t, carry):
            rows = pl.ds(pl.multiple_of(t * 8, 8), 8)
            s, q, r = carry
            for c in range(width // 128):
                lanes = slice(c * 128, (c + 1) * 128)
                a = mix(low, range(group), rows, lanes)
                b = mix(top, range(group, 2 * group), rows, lanes)
                node[0, rows, lanes] = a
                node[1, rows, lanes] = b
                s, q, r = s + a * b, q + a * a, r + b * b
            return s, q, r

        s, q, r = lax.fori_loop(0, block // 8, strip, (zero,) * 3)
        sums3[...] = row_of([s, q, r])

    finish3, sent3 = gather(slots3, slot3_send, slot3_recv, slots3[dp * 2 + core])
    line = finish3()
    s = lane_value(line, 0)
    low = jnp.broadcast_to(1.0 - s / (2.0 * (lane_value(line, 1) + epsilon)), (8, width))
    top = jnp.broadcast_to(1.0 - s / (2.0 * (lane_value(line, 2) + epsilon)), (8, width))

    def last(first, second, other):
        def strip(t, carry):
            rows = pl.ds(pl.multiple_of(t * 8, 8), 8)
            comb[rows, :] = first * node[0, rows, :] + second * other[rows, :]
            return carry
        lax.fori_loop(0, block // 8, strip, 0)

    @pl.when(edge)
    def _():
        last((1.0 - up) * low + up * top, up * low + (1.0 - up) * top, arrived)

    @pl.when(mid)
    def _():
        last(low, top, node.at[1])

    mate_copy(dp, core).wait_send()
    for k in range(len(landed)):
        for i in landed[k][0]:
            mate_copy(spot(*i), core).wait_send()
        if k < len(common):
            for c in og_wave(k, common):
                c.wait_send()
    part.wait_send()

    @pl.when(mid)
    def _():
        for k in range(len(landed)):
            for i in landed[k][1]:
                mate_copy(spot(*i), core).wait_send()
            if k < len(common):
                for c in og_wave(k, extra):
                    c.wait_send()
                for kind, m in plan(k, 1):
                    act_copy(kind, m).wait_send()

    @pl.when(edge)
    def _():
        for k in range(len(common)):
            for kind, m in plan(k, 0):
                act_copy(kind, m).wait_send()
        for k in range(pieces):
            node_copy(k).wait_send()

    sent()
    sent3()


ORDER = (3, 1, 0, 2)
BATCHES = (
    (
        ((3, 4),),
        (
            (3, 5), (3, 6), (3, 7), (2, 4), (2, 5), (2, 6), (2, 7),
            (0, 3), (0, 2), (0, 1), (1, 3), (1, 2), (1, 1),
        ),
    ),
    (
        ((3, 4), (0, 4)),
        (
            (3, 5), (0, 5), (3, 6), (0, 6), (3, 7), (0, 7), (1, 4), (1, 5), (1, 6), (1, 7),
            (2, 3), (2, 2), (2, 1),
        ),
    ),
)


def exchange(n_dp, pre_act, out_weight, out_grad):
    tokens, hidden = pre_act.shape
    block = hidden // n_dp
    width = out_grad.shape[1]
    own_rows = out_grad.shape[0]
    step_cols = hidden // 8
    pieces = 4
    dma = pltpu.SemaphoreType.DMA
    hbm = pl.BlockSpec(memory_space=pl.ANY)
    vmem = pl.BlockSpec(memory_space=pltpu.VMEM)
    return pl.pallas_call(
        functools.partial(kernel, n_dp),
        out_shape=(
            jax.ShapeDtypeStruct((own_rows, width), jnp.bfloat16),
            jax.ShapeDtypeStruct((block, width), jnp.float32),
        ),
        in_specs=[hbm, hbm, hbm],
        out_specs=(vmem, vmem),
        scratch_shapes=[
            pltpu.VMEM((n_dp, tokens, block), jnp.bfloat16),
            pltpu.VMEM((n_dp, tokens, width), jnp.bfloat16),
            pltpu.VMEM((n_dp, block, width), jnp.float32),
            pltpu.VMEM((2, block, width), jnp.float32),
            pltpu.VMEM((block, width), jnp.float32),
            pltpu.VMEM((2, tokens, step_cols), jnp.bfloat16),
            pltpu.VMEM((2, step_cols, width), jnp.bfloat16),
            pltpu.VMEM((tokens, width), jnp.float32),
            pltpu.VMEM((own_rows, width), jnp.float32),
            pltpu.VMEM((128, 128), jnp.float32),
            pltpu.VMEM((2 * n_dp, 1, 128), jnp.float32),
            pltpu.VMEM((2 * n_dp, 1, 128), jnp.float32),
            pltpu.VMEM((n_dp, 128), jnp.float32),
            dma((16,)), dma((n_dp,)), dma((16,)), dma((n_dp,)), dma((n_dp,)), dma((n_dp,)), dma,
            dma((2, 2)), dma((2,)), dma((2 * n_dp,)), dma((2 * n_dp,)),
            dma((pieces,)), dma((pieces,)), dma((2 * n_dp,)), dma((2 * n_dp,)),
        ],
        compiler_params=pltpu.CompilerParams(
            collective_id=0, has_side_effects=True, vmem_limit_bytes=60 * 2**20
        ),
    )(pre_act, out_weight, out_grad)


def local(pre_act, out_weight, out_grad):
    n_dp = lax.axis_size("dp")
    block = pre_act.shape[1] // n_dp
    rows = out_grad.shape[0]
    if lax.axis_size("mp") == 2 and n_dp == 4 * len(ORDER) and block % 128 == 0 and rows % 16 == 0:
        return exchange(n_dp, pre_act, out_weight, out_grad)
    return halving(pre_act, out_weight, out_grad)


def solution(mesh):
    placed = (P("dp", "mp"), P("mp", None), P(("dp", "mp"), None))
    return jax.shard_map(
        local,
        mesh=mesh,
        in_specs=placed,
        out_specs=(P(("dp", "mp"), None), P(("mp", "dp"), None)),
        check_vma=False,
    )
```

```python
import functools
import jax
import jax.numpy as jnp
from jax import lax
from jax.experimental import pallas as pl
from jax.experimental.pallas import tpu as pltpu
from jax.sharding import PartitionSpec as P

epsilon = 1e-06
MESH = pl.DeviceIdType.MESH


def from_partner(value, axis, apart):
    mask = 2**apart
    pairs = [(source, source ^ mask) for source in range(lax.axis_size(axis))]
    return lax.ppermute(value, axis, pairs)


def contract(left, right):
    return lax.dot_general(
        left, right, (((0,), (0,)), ((), ())), preferred_element_type=jnp.float32
    )


def split_rows(piece, block, which):
    width = piece.shape[1]
    blocks = piece.reshape(piece.shape[0] // (2 * block), 2, block, width)
    kept = lax.dynamic_index_in_dim(blocks, which, 1, False).reshape(-1, width)
    sent = lax.dynamic_index_in_dim(blocks, 1 - which, 1, False).reshape(-1, width)
    return (kept, sent)


def level_sums(partial_value, level):
    totals = lax.psum(partial_value, "mp")
    for inner_bit in range(level + 1):
        totals = totals + from_partner(totals, "dp", inner_bit)
    return totals


def merge_level(own, other, level, which):
    lower = which == 0
    own_sq = jnp.sum(own * own)
    other_sq = jnp.sum(other * other)
    partial_value = jnp.stack(
        [
            jnp.sum(own * other),
            jnp.where(lower, own_sq, other_sq),
            jnp.where(lower, other_sq, own_sq),
        ]
    )
    totals = level_sums(partial_value, level)
    first_coef = 1.0 - totals[0] / (2.0 * (totals[1] + epsilon))
    second_coef = 1.0 - totals[0] / (2.0 * (totals[2] + epsilon))
    own_coef = jnp.where(lower, first_coef, second_coef)
    other_coef = jnp.where(lower, second_coef, first_coef)
    return own_coef * own + other_coef * other


def halving(pre_act, out_weight, out_grad):
    act = jnp.maximum(pre_act, jnp.zeros((), jnp.bfloat16))
    tokens = act.shape[0]
    partial_out = jnp.dot(act, out_weight, preferred_element_type=jnp.float32)
    summed = lax.psum_scatter(partial_out, "mp", scatter_dimension=0, tiled=True)
    projected = summed.astype(jnp.bfloat16)
    grad_full = lax.all_gather(out_grad, "mp", axis=0, tiled=True)
    count = lax.axis_size("dp")
    levels = count.bit_length() - 1
    me = lax.axis_index("dp")
    block = act.shape[1] // count
    first_bit = me & 1
    groups = act.reshape(tokens, act.shape[1] // (2 * block), 2, block)
    kept_act = lax.dynamic_index_in_dim(groups, first_bit, 2, False).reshape(tokens, -1)
    sent_act = lax.dynamic_index_in_dim(groups, 1 - first_bit, 2, False).reshape(tokens, -1)
    packed = jnp.concatenate([sent_act, grad_full], axis=1)
    arrived = from_partner(packed, "dp", 0)
    half = sent_act.shape[1]
    own = contract(kept_act, grad_full)
    other = contract(arrived[:, :half], arrived[:, half:])
    piece = merge_level(own, other, 0, first_bit)
    for level in range(1, levels):
        which = me >> level & 1
        own, sent = split_rows(piece, block, which)
        other = from_partner(sent, "dp", level)
        piece = merge_level(own, other, level, which)
    return (projected, piece)


def row_of(values):
    parts = [jnp.sum(v, axis=0, keepdims=True) for v in values]
    parts += [jnp.zeros_like(parts[0])] * (8 - len(parts))
    table = jnp.concatenate(parts, axis=0)
    return line_of(table)


def line_of(table):
    totals = jnp.sum(table, axis=1, keepdims=True)
    lane = lax.broadcasted_iota(jnp.int32, table.shape, 1)
    row = lax.broadcasted_iota(jnp.int32, table.shape, 0)
    return jnp.sum(jnp.where(lane == row, totals, 0.0), axis=0, keepdims=True)


def lane_value(line, p):
    lane = lax.broadcasted_iota(jnp.int32, line.shape, 1)
    return jnp.sum(jnp.where(lane == p, line, 0.0), axis=1, keepdims=True)


def swap(value, axis, bit):
    size = value.shape[axis]
    at = lax.broadcasted_iota(jnp.int32, value.shape, axis)
    up = pltpu.roll(value, size - bit, axis)
    down = pltpu.roll(value, bit, axis)
    return jnp.where((at // bit) % 2 == 0, up, down)


def tree_coefs(line, group):
    rows = 2 * group
    lanes = line.shape[1]
    m = jnp.concatenate([pltpu.roll(jnp.broadcast_to(line, (8, lanes)), group * r, 1)[0:1] if r else line for r in range(rows)], axis=0)
    lane = lax.broadcasted_iota(jnp.int32, m.shape, 1)
    own = lax.broadcasted_iota(jnp.int32, m.shape, 0) % group
    coef = jnp.ones_like(m)
    for level in range(group.bit_length() - 1):
        bit = 2**level
        mate = jnp.where((own // bit) % 2 == 0, own + bit, own - bit)
        inner = jnp.sum(jnp.where(lane == mate, m, 0.0), axis=1, keepdims=True)
        square = jnp.sum(jnp.where(lane == own, m, 0.0), axis=1, keepdims=True)
        f = 1.0 - inner / (2.0 * (jnp.maximum(square, 0.0) + epsilon))
        f = jnp.broadcast_to(f, m.shape)
        coef = coef * f
        across = jnp.where(lane == own, f, 0.0)
        across = jnp.concatenate(
            [jnp.broadcast_to(jnp.sum(across[g * group:(g + 1) * group], axis=0, keepdims=True), (group, lanes)) for g in range(2)],
            axis=0,
        )
        m = m * f * across
        m = m + swap(m, 1, bit)
        m = m + swap(m, 0, bit)
    return coef


def kernel(
    n_dp, pre, w, og, proj, comb,
    acts, grads, leaf, node, arrived, xbuf, wbuf, acc, part_in, gsum, slots, slots3, coefs,
    act_send, act_recv, og_send, og_recv, mate_send, mate_recv, local_sem,
    fwd_sem, part_sem, slot_send, slot_recv, node_send, node_recv, slot3_send, slot3_recv, ready,
):
    dp = lax.axis_index("dp")
    core = lax.axis_index("mp")
    group = n_dp // 2
    me = lax.rem(dp, group)
    z = dp // 4
    y = lax.rem(dp // 2, 2)
    x = lax.rem(dp, 2)
    high = z // 2
    zi = 2 * high + 1 - lax.rem(z, 2)
    tokens = pre.shape[0]
    block = pre.shape[1] // n_dp
    own_rows = og.shape[0]
    width = og.shape[1]
    mate = 1 - core
    edge_z, mid_z = 3 * high, 1 + high
    far_edge_z, far_mid_z = 3 - 3 * high, 2 - high
    edge = z == edge_z
    mid = z == mid_z

    def spot(at_z, m):
        dx = lax.rem(m, 2) if not isinstance(m, int) else m % 2
        dy = m // 2
        return at_z * 4 + (y + dy - 2 * dy * y) * 2 + x + dx - 2 * dx * x

    def turn(j):
        k = core * (ORDER[(j + 2) % 4] - ORDER[j]) + ORDER[j]
        return k

    barrier = pltpu.get_barrier_semaphore()

    def greet(sem, to, side):
        pl.semaphore_signal(sem, inc=1, device_id=(to, side), device_id_type=MESH)

    beside, behind, above, across = spot(z, 1), spot(z, 2), spot(zi, 0), spot(far_mid_z, 0)
    for to in (beside, behind, above):
        greet(barrier, to, core)
    greet(barrier, dp, mate)

    @pl.when(mid)
    def _():
        greet(barrier, across, core)

    def half(i, side):
        return grads.at[i, pl.ds(side * own_rows, own_rows)]

    home = dp
    og_local = pltpu.make_async_copy(og, half(dp, core), local_sem)
    og_local.start()

    def cols(b):
        return pl.ds(pl.multiple_of(b * block, block), block)

    def self_copy(b, slot):
        return pltpu.make_async_copy(pre.at[:, cols(b)], acts.at[slot], act_recv.at[slot])

    step_cols = xbuf.shape[2]
    steps = pre.shape[1] // step_cols

    def fetch(k, slot):
        here = pl.ds(pl.multiple_of(k * step_cols, step_cols), step_cols)
        return (
            pltpu.make_async_copy(pre.at[:, here], xbuf.at[slot], fwd_sem.at[slot, 0]),
            pltpu.make_async_copy(w.at[here, :], wbuf.at[slot], fwd_sem.at[slot, 1]),
        )

    for c in fetch(0, 0):
        c.start()
    acc[...] = jnp.zeros_like(acc)
    gsum[...] = jnp.zeros_like(gsum)

    def og_copy(n, i, to):
        return pltpu.make_async_remote_copy(
            src_ref=og if i is home else half(i, core), dst_ref=half(i, core), send_sem=og_send.at[n],
            recv_sem=og_recv.at[i], device_id=(to, core), device_id_type=MESH,
        )

    def mate_copy(i, side):
        return pltpu.make_async_remote_copy(
            src_ref=half(i, side), dst_ref=half(i, side), send_sem=mate_send.at[i],
            recv_sem=mate_recv.at[i], device_id=(dp, mate), device_id_type=MESH,
        )

    def og_arrival(i):
        og_copy(0, i, dp).wait_recv()
        mate_copy(i, core).start()

    def act_copy(kind, m):
        if kind < 2:
            to = spot(edge_z, m)
            b, slot = (to if kind == 0 else spot(far_edge_z, m)), me * 2 + kind
        else:
            to = spot(mid_z if kind == 2 else far_mid_z, m)
            b, slot = to, dp
        return pltpu.make_async_remote_copy(
            src_ref=pre.at[:, cols(b)], dst_ref=acts.at[slot],
            send_sem=act_send.at[kind * 4 + m], recv_sem=act_recv.at[slot],
            device_id=(to, core), device_id_type=MESH,
        )

    def plan(batch, where):
        return [(kind, turn(m - 4) if m > 3 else m) for kind, m in BATCHES[where][batch]]

    def send_acts(batch):
        for where, here in ((0, edge), (1, mid)):
            @pl.when(here)
            def _():
                for kind, m in plan(batch, where):
                    act_copy(kind, m).start()

    def meet(n, to, side):
        greet(ready.at[n], to, side)
        pl.semaphore_wait(ready.at[n], 1)

    common = (
        ((z, 0, zi, 0), (z, 0, z, 1), (z, 0, z, 2), (z, 0, far_mid_z, 0), (z, 0, z, 3)),
        ((z, 1, zi, 0), (z, 2, zi, 0), (z, 3, zi, 0)),
    )
    extra = (
        (),
        (
            (z, 1, far_mid_z, 0), (z, 2, far_mid_z, 0), (z, 3, far_mid_z, 0),
            (far_edge_z, 0, z, 3), (far_edge_z, 0, z, 1), (far_edge_z, 0, z, 2),
        ),
    )
    landed = (
        ((), ()),
        (((z, 1), (z, 2), (z, 3), (zi, 0)), ((far_mid_z, 0), (far_edge_z, 0))),
        (
            ((zi, 1), (zi, 2), (zi, 3)),
            tuple((far_mid_z, m) for m in (1, 2, 3)) + tuple((far_edge_z, m) for m in (1, 2, 3)),
        ),
    )

    def og_wave(k, moves):
        base = sum(len(c) for c in moves[:k])
        base += sum(len(c) for c in common) if moves is extra else 0
        return [og_copy(base + n, home if a is z and m == 0 else spot(a, m), spot(b, r)) for n, (a, m, b, r) in enumerate(moves[k])]

    def wave(k):
        for i in landed[k][0]:
            og_arrival(spot(*i))

        @pl.when(mid)
        def _():
            for i in landed[k][1]:
                og_arrival(spot(*i))

        if k < len(common):
            for c in og_wave(k, common):
                c.start()

            @pl.when(mid)
            def _():
                for c in og_wave(k, extra):
                    c.start()

            send_acts(k)

    first = og_wave(0, common)

    @pl.when(edge)
    def _():
        pl.semaphore_wait(barrier, 4)

    @pl.when(mid)
    def _():
        pl.semaphore_wait(barrier, 5)
        first[3].start()

    for c in first[:3]:
        c.start()
    og_local.wait()
    mate_copy(dp, core).start()
    meet(0, beside, core)
    meet(1, behind, core)
    first[4].start()
    meet(2, dp, mate)

    @pl.when(mid)
    def _():
        meet(3, across, core)

    meet(4, above, core)

    @pl.when(edge)
    def _():
        first[3].start()

    send_acts(0)

    @pl.when(edge)
    def _():
        self_copy(dp, me * 2).start()
        self_copy(spot(far_edge_z, 0), me * 2 + 1).start()

    @pl.when(mid)
    def _():
        self_copy(dp, dp).start()

    def forward(k, carry):
        slot = lax.rem(k, 2)

        @pl.when(k + 1 < steps)
        def _():
            for c in fetch(k + 1, 1 - slot):
                c.start()

        for c in fetch(k, slot):
            c.wait()
        v = jnp.maximum(xbuf[slot], jnp.zeros((), jnp.bfloat16))
        acc[...] += jnp.dot(v, wbuf[slot], preferred_element_type=jnp.float32)
        return carry

    lax.fori_loop(0, steps, forward, 0)
    part = pltpu.make_async_remote_copy(
        src_ref=acc.at[pl.ds(mate * own_rows, own_rows)], dst_ref=part_in,
        send_sem=part_sem.at[0], recv_sem=part_sem.at[1],
        device_id=(dp, mate), device_id_type=MESH,
    )
    part.start()
    wave(1)
    part.wait_recv()
    proj[...] = (acc[pl.ds(core * own_rows, own_rows), :] + part_in[...]).astype(proj.dtype)
    wave(2)

    def settle(i):
        mate_copy(i, mate).wait_recv()

    def leaf_grad(i, slot, own):
        if own:
            self_copy(0, slot).wait()
        else:
            pltpu.make_async_remote_copy(
                src_ref=pre.at[:, cols(0)], dst_ref=acts.at[slot], send_sem=act_send.at[0],
                recv_sem=act_recv.at[slot], device_id=(dp, mate), device_id_type=MESH,
            ).wait_recv()
        a = jnp.maximum(acts[slot], jnp.zeros((), jnp.bfloat16))
        leaf[slot] = contract(a, grads[i])

    def gram(new, others):
        i, slot = new
        seen = others + [new]

        def strip(t, carry):
            rows = pl.ds(pl.multiple_of(t * 8, 8), 8)
            for c in range(width // 128):
                lanes = slice(c * 128, (c + 1) * 128)
                v = leaf[slot, rows, lanes]
                carry = tuple(s + v * leaf[o, rows, lanes] for s, (_, o) in zip(carry, seen[:-1])) + (carry[-1] + v * v,)
            return carry

        zero = jnp.zeros((8, 128), jnp.float32)
        sums = lax.fori_loop(0, block // 8, strip, (zero,) * len(seen))
        for s, (j, _) in zip(sums, seen):
            line = jnp.sum(s, axis=0, keepdims=True)
            for p, q in ((i, j), (j, i))[: 1 if j is i else 2]:
                at = pl.ds(lax.rem(2 * group - p, 2 * group) * group + lax.rem(q, group), 1)
                gsum[at, :] += line

    @pl.when(edge)
    def _():
        def both(h, carry):
            done = []
            for n, (at_z, m) in enumerate([(z, 0), (z, 3), (z, 2), (z, 1)] + [(zi, turn(j)) for j in range(4)]):
                i = spot(at_z, m)

                @pl.when(h == 0)
                def _():
                    settle(i)

                slot = lax.rem(i, group) * 2 + h
                leaf_grad(i, slot, n == 0)
                gram((i, slot), done)
                done = done + [(i, slot)]
            return carry

        lax.fori_loop(0, 2, both, 0)

    @pl.when(mid)
    def _():
        near, away = [], []

        def take(i, seen):
            settle(i)
            leaf_grad(i, i, i is home)
            gram((i, i), seen)
            seen.append((i, i))

        take(home, near)
        for m in (3, 2, 1):
            take(spot(z, m), near)
        for j in range(4):
            take(spot(far_edge_z, turn(j)), away)
        for j in range(4):
            take(spot(far_mid_z, turn(j)), away)
            take(spot(zi, turn(j)), near)

    def gather(buf, send, recv, line):
        mine = dp * 2 + core
        buf[mine] = line

        def copy(q, other, at):
            return pltpu.make_async_remote_copy(
                src_ref=buf.at[at], dst_ref=buf.at[at], send_sem=send.at[q], recv_sem=recv.at[at],
                device_id=(other // 2, lax.rem(other, 2)), device_id_type=MESH,
            )

        def go(q, carry):
            copy(q, lax.rem(mine + q, 2 * n_dp), mine).start()
            return carry

        def left(q, carry):
            copy(q, lax.rem(mine + q, 2 * n_dp), mine).wait_send()
            return carry

        def settled(first, count):
            def take(k, carry):
                @pl.when(first + k != mine)
                def _():
                    copy(0, first + k, first + k).wait_recv()
                return carry

            lax.fori_loop(0, count, take, 0)

        def finish(first, count):
            settled(first, count)
            total = buf[first]
            for k in range(1, count):
                total = total + buf[first + k]
            return total

        lax.fori_loop(n_dp, 2 * n_dp, go, 0)
        lax.fori_loop(1, n_dp, go, 0)
        return finish, settled, lambda: lax.fori_loop(1, 2 * n_dp, left, 0)

    finish, settled, sent = gather(slots, slot_send, slot_recv, line_of(gsum[...]))
    plane = n_dp // 2

    @pl.when(edge)
    def _():
        coefs[...] = tree_coefs(finish(high * plane, 3 * plane), group)

    @pl.when(mid)
    def _():
        coefs[...] = tree_coefs(finish(0, 2 * n_dp), group)

    def weights(first):
        return [jnp.broadcast_to(coefs[pl.ds(first + k, 1), :], (8, 128)) for k in range(group)]

    pieces = node_send.shape[0]
    tall = block // pieces

    def mix(weight, places, rows, lanes):
        total = weight[0] * leaf[places[0], rows, lanes]
        for k in range(1, group):
            total = total + weight[k] * leaf[places[k], rows, lanes]
        return total

    zero = jnp.zeros((8, 128), jnp.float32)
    far = spot(far_edge_z, 0)

    def node_copy(k):
        rows = pl.ds(k * tall, tall)
        return pltpu.make_async_remote_copy(
            src_ref=node.at[1, rows], dst_ref=arrived.at[rows],
            send_sem=node_send.at[k], recv_sem=node_recv.at[k],
            device_id=(far, core), device_id_type=MESH,
        )

    sums3 = slots3.at[dp * 2 + core]
    up = high.astype(jnp.float32)

    @pl.when(edge)
    def _():
        weight = weights(high * group)

        def build(h, first, count, q):
            def strip(t, q):
                rows = pl.ds(pl.multiple_of(first + t * 8, 8), 8)
                for c in range(width // 128):
                    lanes = slice(c * 128, (c + 1) * 128)
                    total = mix(weight, [2 * k + h for k in range(group)], rows, lanes)
                    node[h, rows, lanes] = total
                    q = q + total * total
                return q
            return lax.fori_loop(0, count // 8, strip, q)

        q = zero
        for k in range(pieces):
            q = build(1, k * tall, tall, q)
            node_copy(k).start()
        q = build(0, 0, block, q)
        s = zero
        for k in range(pieces):
            node_copy(k).wait_recv()

            def inner(t, s):
                rows = pl.ds(pl.multiple_of(k * tall + t * 8, 8), 8)
                for c in range(width // 128):
                    lanes = slice(c * 128, (c + 1) * 128)
                    s = s + node[0, rows, lanes] * arrived[rows, lanes]
                return s

            s = lax.fori_loop(0, tall // 8, inner, s)
        sums3[...] = row_of([s, (1.0 - up) * q, up * q])

    @pl.when(mid)
    def _():
        low, top = weights(0), weights(group)

        def strip(t, carry):
            rows = pl.ds(pl.multiple_of(t * 8, 8), 8)
            s, q, r = carry
            for c in range(width // 128):
                lanes = slice(c * 128, (c + 1) * 128)
                a = mix(low, range(group), rows, lanes)
                b = mix(top, range(group, 2 * group), rows, lanes)
                node[0, rows, lanes] = a
                node[1, rows, lanes] = b
                s, q, r = s + a * b, q + a * a, r + b * b
            return s, q, r

        s, q, r = lax.fori_loop(0, block // 8, strip, (zero,) * 3)
        sums3[...] = row_of([s, q, r])

    finish3, _, sent3 = gather(slots3, slot3_send, slot3_recv, slots3[dp * 2 + core])
    line = finish3(0, 2 * n_dp)
    s = lane_value(line, 0)
    low = jnp.broadcast_to(1.0 - s / (2.0 * (lane_value(line, 1) + epsilon)), (8, width))
    top = jnp.broadcast_to(1.0 - s / (2.0 * (lane_value(line, 2) + epsilon)), (8, width))

    def last(first, second, other):
        def strip(t, carry):
            rows = pl.ds(pl.multiple_of(t * 8, 8), 8)
            comb[rows, :] = first * node[0, rows, :] + second * other[rows, :]
            return carry
        lax.fori_loop(0, block // 8, strip, 0)

    @pl.when(edge)
    def _():
        last((1.0 - up) * low + up * top, up * low + (1.0 - up) * top, arrived)

    @pl.when(mid)
    def _():
        last(low, top, node.at[1])

    @pl.when(edge)
    def _():
        settled(far_edge_z * plane, plane)

    mate_copy(dp, core).wait_send()
    for k in range(len(landed)):
        for i in landed[k][0]:
            mate_copy(spot(*i), core).wait_send()
        if k < len(common):
            for c in og_wave(k, common):
                c.wait_send()
    part.wait_send()

    @pl.when(mid)
    def _():
        for k in range(len(landed)):
            for i in landed[k][1]:
                mate_copy(spot(*i), core).wait_send()
            if k < len(common):
                for c in og_wave(k, extra):
                    c.wait_send()
                for kind, m in plan(k, 1):
                    act_copy(kind, m).wait_send()

    @pl.when(edge)
    def _():
        for k in range(len(common)):
            for kind, m in plan(k, 0):
                act_copy(kind, m).wait_send()
        for k in range(pieces):
            node_copy(k).wait_send()

    sent()
    sent3()


ORDER = (3, 1, 0, 2)
BATCHES = (
    (
        ((3, 4),),
        (
            (3, 5), (3, 6), (3, 7), (2, 4), (2, 5), (2, 6), (2, 7),
            (0, 3), (0, 2), (0, 1), (1, 3), (1, 2), (1, 1),
        ),
    ),
    (
        ((3, 4), (0, 4)),
        (
            (3, 5), (0, 5), (3, 6), (0, 6), (3, 7), (0, 7), (1, 4), (1, 5), (1, 6), (1, 7),
            (2, 3), (2, 2), (2, 1),
        ),
    ),
)


def exchange(n_dp, pre_act, out_weight, out_grad):
    tokens, hidden = pre_act.shape
    block = hidden // n_dp
    width = out_grad.shape[1]
    own_rows = out_grad.shape[0]
    step_cols = hidden // 8
    pieces = 4
    dma = pltpu.SemaphoreType.DMA
    hbm = pl.BlockSpec(memory_space=pl.ANY)
    vmem = pl.BlockSpec(memory_space=pltpu.VMEM)
    return pl.pallas_call(
        functools.partial(kernel, n_dp),
        out_shape=(
            jax.ShapeDtypeStruct((own_rows, width), jnp.bfloat16),
            jax.ShapeDtypeStruct((block, width), jnp.float32),
        ),
        in_specs=[hbm, hbm, hbm],
        out_specs=(vmem, vmem),
        scratch_shapes=[
            pltpu.VMEM((n_dp, tokens, block), jnp.bfloat16),
            pltpu.VMEM((n_dp, tokens, width), jnp.bfloat16),
            pltpu.VMEM((n_dp, block, width), jnp.float32),
            pltpu.VMEM((2, block, width), jnp.float32),
            pltpu.VMEM((block, width), jnp.float32),
            pltpu.VMEM((2, tokens, step_cols), jnp.bfloat16),
            pltpu.VMEM((2, step_cols, width), jnp.bfloat16),
            pltpu.VMEM((tokens, width), jnp.float32),
            pltpu.VMEM((own_rows, width), jnp.float32),
            pltpu.VMEM((128, 128), jnp.float32),
            pltpu.VMEM((2 * n_dp, 1, 128), jnp.float32),
            pltpu.VMEM((2 * n_dp, 1, 128), jnp.float32),
            pltpu.VMEM((n_dp, 128), jnp.float32),
            dma((16,)), dma((n_dp,)), dma((16,)), dma((n_dp,)), dma((n_dp,)), dma((n_dp,)), dma,
            dma((2, 2)), dma((2,)), dma((2 * n_dp,)), dma((2 * n_dp,)),
            dma((pieces,)), dma((pieces,)), dma((2 * n_dp,)), dma((2 * n_dp,)),
            pltpu.SemaphoreType.REGULAR((5,)),
        ],
        compiler_params=pltpu.CompilerParams(
            collective_id=0, has_side_effects=True, vmem_limit_bytes=52 * 2**20
        ),
    )(pre_act, out_weight, out_grad)


def local(pre_act, out_weight, out_grad):
    n_dp = lax.axis_size("dp")
    block = pre_act.shape[1] // n_dp
    rows = out_grad.shape[0]
    if lax.axis_size("mp") == 2 and n_dp == 4 * len(ORDER) and block % 128 == 0 and rows % 16 == 0:
        return exchange(n_dp, pre_act, out_weight, out_grad)
    return halving(pre_act, out_weight, out_grad)


def solution(mesh):
    placed = (P("dp", "mp"), P("mp", None), P(("dp", "mp"), None))
    return jax.shard_map(
        local,
        mesh=mesh,
        in_specs=placed,
        out_specs=(P(("dp", "mp"), None), P(("mp", "dp"), None)),
        check_vma=False,
    )
```

```python
import functools
import jax
import jax.numpy as jnp
from jax import lax
from jax.experimental import pallas as pl
from jax.experimental.pallas import tpu as pltpu
from jax.sharding import PartitionSpec as P

epsilon = 1e-06
MESH = pl.DeviceIdType.MESH


def from_partner(value, axis, apart):
    mask = 2**apart
    pairs = [(source, source ^ mask) for source in range(lax.axis_size(axis))]
    return lax.ppermute(value, axis, pairs)


def contract(left, right):
    return lax.dot_general(
        left, right, (((0,), (0,)), ((), ())), preferred_element_type=jnp.float32
    )


def split_rows(piece, block, which):
    width = piece.shape[1]
    blocks = piece.reshape(piece.shape[0] // (2 * block), 2, block, width)
    kept = lax.dynamic_index_in_dim(blocks, which, 1, False).reshape(-1, width)
    sent = lax.dynamic_index_in_dim(blocks, 1 - which, 1, False).reshape(-1, width)
    return (kept, sent)


def level_sums(partial_value, level):
    totals = lax.psum(partial_value, "mp")
    for inner_bit in range(level + 1):
        totals = totals + from_partner(totals, "dp", inner_bit)
    return totals


def merge_level(own, other, level, which):
    lower = which == 0
    own_sq = jnp.sum(own * own)
    other_sq = jnp.sum(other * other)
    partial_value = jnp.stack(
        [
            jnp.sum(own * other),
            jnp.where(lower, own_sq, other_sq),
            jnp.where(lower, other_sq, own_sq),
        ]
    )
    totals = level_sums(partial_value, level)
    first_coef = 1.0 - totals[0] / (2.0 * (totals[1] + epsilon))
    second_coef = 1.0 - totals[0] / (2.0 * (totals[2] + epsilon))
    own_coef = jnp.where(lower, first_coef, second_coef)
    other_coef = jnp.where(lower, second_coef, first_coef)
    return own_coef * own + other_coef * other


def halving(pre_act, out_weight, out_grad):
    act = jnp.maximum(pre_act, jnp.zeros((), jnp.bfloat16))
    tokens = act.shape[0]
    partial_out = jnp.dot(act, out_weight, preferred_element_type=jnp.float32)
    summed = lax.psum_scatter(partial_out, "mp", scatter_dimension=0, tiled=True)
    projected = summed.astype(jnp.bfloat16)
    grad_full = lax.all_gather(out_grad, "mp", axis=0, tiled=True)
    count = lax.axis_size("dp")
    levels = count.bit_length() - 1
    me = lax.axis_index("dp")
    block = act.shape[1] // count
    first_bit = me & 1
    groups = act.reshape(tokens, act.shape[1] // (2 * block), 2, block)
    kept_act = lax.dynamic_index_in_dim(groups, first_bit, 2, False).reshape(tokens, -1)
    sent_act = lax.dynamic_index_in_dim(groups, 1 - first_bit, 2, False).reshape(tokens, -1)
    packed = jnp.concatenate([sent_act, grad_full], axis=1)
    arrived = from_partner(packed, "dp", 0)
    half = sent_act.shape[1]
    own = contract(kept_act, grad_full)
    other = contract(arrived[:, :half], arrived[:, half:])
    piece = merge_level(own, other, 0, first_bit)
    for level in range(1, levels):
        which = me >> level & 1
        own, sent = split_rows(piece, block, which)
        other = from_partner(sent, "dp", level)
        piece = merge_level(own, other, level, which)
    return (projected, piece)


def row_of(values):
    parts = [jnp.sum(v, axis=0, keepdims=True) for v in values]
    parts += [jnp.zeros_like(parts[0])] * (8 - len(parts))
    table = jnp.concatenate(parts, axis=0)
    return line_of(table)


def line_of(table):
    totals = jnp.sum(table, axis=1, keepdims=True)
    lane = lax.broadcasted_iota(jnp.int32, table.shape, 1)
    row = lax.broadcasted_iota(jnp.int32, table.shape, 0)
    return jnp.sum(jnp.where(lane == row, totals, 0.0), axis=0, keepdims=True)


def lane_value(line, p):
    lane = lax.broadcasted_iota(jnp.int32, line.shape, 1)
    return jnp.sum(jnp.where(lane == p, line, 0.0), axis=1, keepdims=True)


def swap(value, axis, bit):
    size = value.shape[axis]
    at = lax.broadcasted_iota(jnp.int32, value.shape, axis)
    up = pltpu.roll(value, size - bit, axis)
    down = pltpu.roll(value, bit, axis)
    return jnp.where((at // bit) % 2 == 0, up, down)


def tree_coefs(line, group):
    rows = 2 * group
    lanes = line.shape[1]
    m = jnp.concatenate([pltpu.roll(jnp.broadcast_to(line, (8, lanes)), group * r, 1)[0:1] if r else line for r in range(rows)], axis=0)
    lane = lax.broadcasted_iota(jnp.int32, m.shape, 1)
    own = lax.broadcasted_iota(jnp.int32, m.shape, 0) % group
    coef = jnp.ones_like(m)
    for level in range(group.bit_length() - 1):
        bit = 2**level
        mate = jnp.where((own // bit) % 2 == 0, own + bit, own - bit)
        inner = jnp.sum(jnp.where(lane == mate, m, 0.0), axis=1, keepdims=True)
        square = jnp.sum(jnp.where(lane == own, m, 0.0), axis=1, keepdims=True)
        f = 1.0 - inner / (2.0 * (jnp.maximum(square, 0.0) + epsilon))
        f = jnp.broadcast_to(f, m.shape)
        coef = coef * f
        across = jnp.where(lane == own, f, 0.0)
        across = jnp.concatenate(
            [jnp.broadcast_to(jnp.sum(across[g * group:(g + 1) * group], axis=0, keepdims=True), (group, lanes)) for g in range(2)],
            axis=0,
        )
        m = m * f * across
        m = m + swap(m, 1, bit)
        m = m + swap(m, 0, bit)
    return coef


def kernel(
    n_dp, pre, w, og, proj, comb,
    acts, grads, leaf, node, arrived, xbuf, wbuf, acc, part_in, gsum, slots, slots3, coefs,
    act_send, act_recv, og_send, og_recv, mate_send, mate_recv, local_sem,
    fwd_sem, part_sem, slot_send, slot_recv, node_send, node_recv, slot3_send, slot3_recv, ready,
):
    dp = lax.axis_index("dp")
    core = lax.axis_index("mp")
    group = n_dp // 2
    me = lax.rem(dp, group)
    z = dp // 4
    y = lax.rem(dp // 2, 2)
    x = lax.rem(dp, 2)
    high = z // 2
    zi = 2 * high + 1 - lax.rem(z, 2)
    tokens = pre.shape[0]
    block = pre.shape[1] // n_dp
    own_rows = og.shape[0]
    width = og.shape[1]
    mate = 1 - core
    edge_z, mid_z = 3 * high, 1 + high
    far_edge_z, far_mid_z = 3 - 3 * high, 2 - high
    edge = z == edge_z
    mid = z == mid_z

    def spot(at_z, m):
        dx = lax.rem(m, 2) if not isinstance(m, int) else m % 2
        dy = m // 2
        return at_z * 4 + (y + dy - 2 * dy * y) * 2 + x + dx - 2 * dx * x

    def turn(j):
        k = core * (ORDER[(j + 2) % 4] - ORDER[j]) + ORDER[j]
        return k

    barrier = pltpu.get_barrier_semaphore()

    def greet(sem, to, side):
        pl.semaphore_signal(sem, inc=1, device_id=(to, side), device_id_type=MESH)

    beside, behind, above, across = spot(z, 1), spot(z, 2), spot(zi, 0), spot(far_mid_z, 0)
    for to in (beside, behind, above):
        greet(barrier, to, core)
    greet(barrier, dp, mate)

    @pl.when(mid)
    def _():
        greet(barrier, across, core)

    def half(i, side):
        return grads.at[i, pl.ds(side * own_rows, own_rows)]

    home = dp
    og_local = pltpu.make_async_copy(og, half(dp, core), local_sem)
    og_local.start()

    def cols(b):
        return pl.ds(pl.multiple_of(b * block, block), block)

    def self_copy(b, slot):
        return pltpu.make_async_copy(pre.at[:, cols(b)], acts.at[slot], act_recv.at[slot])

    step_cols = xbuf.shape[2]
    steps = pre.shape[1] // step_cols

    def fetch(k, slot):
        here = pl.ds(pl.multiple_of(k * step_cols, step_cols), step_cols)
        return (
            pltpu.make_async_copy(pre.at[:, here], xbuf.at[slot], fwd_sem.at[slot, 0]),
            pltpu.make_async_copy(w.at[here, :], wbuf.at[slot], fwd_sem.at[slot, 1]),
        )

    for c in fetch(0, 0):
        c.start()
    acc[...] = jnp.zeros_like(acc)
    gsum[...] = jnp.zeros_like(gsum)

    def og_copy(n, i, to):
        return pltpu.make_async_remote_copy(
            src_ref=og if i is home else half(i, core), dst_ref=half(i, core), send_sem=og_send,
            recv_sem=og_recv.at[i], device_id=(to, core), device_id_type=MESH,
        )

    def mate_copy(i, side):
        return pltpu.make_async_remote_copy(
            src_ref=half(i, side), dst_ref=half(i, side), send_sem=mate_send,
            recv_sem=mate_recv.at[i], device_id=(dp, mate), device_id_type=MESH,
        )

    def og_arrival(i):
        og_copy(0, i, dp).wait_recv()
        mate_copy(i, core).start()

    def act_copy(kind, m):
        if kind < 2:
            to = spot(edge_z, m)
            b, slot = (to if kind == 0 else spot(far_edge_z, m)), me * 2 + kind
        else:
            to = spot(mid_z if kind == 2 else far_mid_z, m)
            b, slot = to, dp
        return pltpu.make_async_remote_copy(
            src_ref=pre.at[:, cols(b)], dst_ref=acts.at[slot],
            send_sem=act_send, recv_sem=act_recv.at[slot],
            device_id=(to, core), device_id_type=MESH,
        )

    def plan(batch, where):
        return [(kind, turn(m - 4) if m > 3 else m) for kind, m in BATCHES[where][batch]]

    def send_acts(batch):
        for where, here in ((0, edge), (1, mid)):
            @pl.when(here)
            def _():
                for kind, m in plan(batch, where):
                    act_copy(kind, m).start()

    def meet(n, to, side):
        greet(ready.at[n], to, side)
        pl.semaphore_wait(ready.at[n], 1)

    common = (
        ((z, 0, zi, 0), (z, 0, z, 1), (z, 0, z, 2), (z, 0, far_mid_z, 0), (z, 0, z, 3)),
        ((z, 1, zi, 0), (z, 2, zi, 0), (z, 3, zi, 0)),
    )
    extra = (
        (),
        (
            (z, 1, far_mid_z, 0), (z, 2, far_mid_z, 0), (z, 3, far_mid_z, 0),
            (far_edge_z, 0, z, 3), (far_edge_z, 0, z, 1), (far_edge_z, 0, z, 2),
        ),
    )
    landed = (
        ((), ()),
        (((z, 1), (z, 2), (z, 3), (zi, 0)), ((far_mid_z, 0), (far_edge_z, 0))),
        (
            ((zi, 1), (zi, 2), (zi, 3)),
            tuple((far_mid_z, m) for m in (1, 2, 3)) + tuple((far_edge_z, m) for m in (1, 2, 3)),
        ),
    )

    def og_wave(k, moves):
        base = sum(len(c) for c in moves[:k])
        base += sum(len(c) for c in common) if moves is extra else 0
        return [og_copy(base + n, home if a is z and m == 0 else spot(a, m), spot(b, r)) for n, (a, m, b, r) in enumerate(moves[k])]

    def wave(k):
        for i in landed[k][0]:
            og_arrival(spot(*i))

        @pl.when(mid)
        def _():
            for i in landed[k][1]:
                og_arrival(spot(*i))

        if k < len(common):
            for c in og_wave(k, common):
                c.start()

            @pl.when(mid)
            def _():
                for c in og_wave(k, extra):
                    c.start()

            send_acts(k)

    first = og_wave(0, common)

    @pl.when(edge)
    def _():
        pl.semaphore_wait(barrier, 4)

    @pl.when(mid)
    def _():
        pl.semaphore_wait(barrier, 5)
        first[3].start()

    for c in first[:3]:
        c.start()
    og_local.wait()
    mate_copy(dp, core).start()
    meet(0, above, core)

    @pl.when(edge)
    def _():
        first[3].start()

    meet(1, beside, core)
    meet(2, behind, core)
    first[4].start()
    send_acts(0)

    @pl.when(edge)
    def _():
        self_copy(dp, me * 2).start()
        self_copy(spot(far_edge_z, 0), me * 2 + 1).start()

    @pl.when(mid)
    def _():
        self_copy(dp, dp).start()

    def forward(k, carry):
        slot = lax.rem(k, 2)

        @pl.when(k + 1 < steps)
        def _():
            for c in fetch(k + 1, 1 - slot):
                c.start()

        for c in fetch(k, slot):
            c.wait()
        v = jnp.maximum(xbuf[slot], jnp.zeros((), jnp.bfloat16))
        acc[...] += jnp.dot(v, wbuf[slot], preferred_element_type=jnp.float32)
        return carry

    lax.fori_loop(0, steps, forward, 0)
    part = pltpu.make_async_remote_copy(
        src_ref=acc.at[pl.ds(mate * own_rows, own_rows)], dst_ref=part_in,
        send_sem=part_sem.at[0], recv_sem=part_sem.at[1],
        device_id=(dp, mate), device_id_type=MESH,
    )
    part.start()
    wave(1)
    meet(3, dp, mate)

    @pl.when(mid)
    def _():
        meet(4, across, core)

    meet(5, above, core)
    part.wait_recv()
    proj[...] = (acc[pl.ds(core * own_rows, own_rows), :] + part_in[...]).astype(proj.dtype)
    wave(2)

    def settle(i):
        mate_copy(i, mate).wait_recv()

    def leaf_grad(i, slot, own):
        if own:
            self_copy(0, slot).wait()
        else:
            pltpu.make_async_remote_copy(
                src_ref=pre.at[:, cols(0)], dst_ref=acts.at[slot], send_sem=act_send,
                recv_sem=act_recv.at[slot], device_id=(dp, mate), device_id_type=MESH,
            ).wait_recv()
        a = jnp.maximum(acts[slot], jnp.zeros((), jnp.bfloat16))
        leaf[slot] = contract(a, grads[i])

    def gram(new, others):
        i, slot = new
        seen = others + [new]

        def strip(t, carry):
            rows = pl.ds(pl.multiple_of(t * 8, 8), 8)
            for c in range(width // 128):
                lanes = slice(c * 128, (c + 1) * 128)
                v = leaf[slot, rows, lanes]
                carry = tuple(s + v * leaf[o, rows, lanes] for s, (_, o) in zip(carry, seen[:-1])) + (carry[-1] + v * v,)
            return carry

        zero = jnp.zeros((8, 128), jnp.float32)
        sums = lax.fori_loop(0, block // 8, strip, (zero,) * len(seen))
        for s, (j, _) in zip(sums, seen):
            line = jnp.sum(s, axis=0, keepdims=True)
            for p, q in ((i, j), (j, i))[: 1 if j is i else 2]:
                at = pl.ds(lax.rem(2 * group - p, 2 * group) * group + lax.rem(q, group), 1)
                gsum[at, :] += line

    @pl.when(edge)
    def _():
        def both(h, carry):
            done = []
            for n, (at_z, m) in enumerate([(z, 0), (z, 3), (z, 2), (z, 1)] + [(zi, turn(j)) for j in range(4)]):
                i = spot(at_z, m)

                @pl.when(h == 0)
                def _():
                    settle(i)

                slot = lax.rem(i, group) * 2 + h
                leaf_grad(i, slot, n == 0)
                gram((i, slot), done)
                done = done + [(i, slot)]
            return carry

        lax.fori_loop(0, 2, both, 0)

    @pl.when(mid)
    def _():
        near, away = [], []

        def take(i, seen):
            settle(i)
            leaf_grad(i, i, i is home)
            gram((i, i), seen)
            seen.append((i, i))

        take(home, near)
        for m in (3, 2, 1):
            take(spot(z, m), near)
        for j in range(4):
            take(spot(far_edge_z, turn(j)), away)
        for j in range(4):
            take(spot(far_mid_z, turn(j)), away)
            take(spot(zi, turn(j)), near)

    plane = n_dp // 2

    def gather(buf, send, recv, line):
        mine = dp * 2 + core
        buf[mine] = line

        def copy(other, at):
            return pltpu.make_async_remote_copy(
                src_ref=buf.at[at], dst_ref=buf.at[at], send_sem=send, recv_sem=recv.at[at // plane],
                device_id=(other // 2, lax.rem(other, 2)), device_id_type=MESH,
            )

        def go(q, carry):
            copy(lax.rem(mine + q, 2 * n_dp), mine).start()
            return carry

        def landing(at_z, rows):
            here = buf.at[pl.ds(0, rows)]
            return pltpu.make_async_remote_copy(
                src_ref=here, dst_ref=here, send_sem=send, recv_sem=recv.at[at_z],
                device_id=(dp, mate), device_id_type=MESH,
            )

        def settled(first, count):
            for k in range(count):
                at_z = first + k

                @pl.when(at_z == z)
                def _():
                    landing(at_z, plane - 1).wait_recv()

                @pl.when(at_z != z)
                def _():
                    landing(at_z, plane).wait_recv()

        def finish(first, count):
            settled(first, count)
            total = buf[first * plane]
            for k in range(1, count * plane):
                total = total + buf[first * plane + k]
            return total

        lax.fori_loop(n_dp, 2 * n_dp, go, 0)
        lax.fori_loop(1, n_dp, go, 0)
        return finish, settled, landing(0, 2 * n_dp - 1).wait_send

    finish, settled, sent = gather(slots, slot_send, slot_recv, line_of(gsum[...]))

    @pl.when(edge)
    def _():
        coefs[...] = tree_coefs(finish(high, 3), group)

    @pl.when(mid)
    def _():
        coefs[...] = tree_coefs(finish(0, 4), group)

    def weights(first):
        return [jnp.broadcast_to(coefs[pl.ds(first + k, 1), :], (8, 128)) for k in range(group)]

    pieces = node_recv.shape[0]
    tall = block // pieces

    def mix(weight, places, rows, lanes):
        total = weight[0] * leaf[places[0], rows, lanes]
        for k in range(1, group):
            total = total + weight[k] * leaf[places[k], rows, lanes]
        return total

    zero = jnp.zeros((8, 128), jnp.float32)
    far = spot(far_edge_z, 0)

    def node_copy(k):
        rows = pl.ds(k * tall, tall)
        return pltpu.make_async_remote_copy(
            src_ref=node.at[1, rows], dst_ref=arrived.at[rows],
            send_sem=node_send, recv_sem=node_recv.at[k],
            device_id=(far, core), device_id_type=MESH,
        )

    sums3 = slots3.at[dp * 2 + core]
    up = high.astype(jnp.float32)

    @pl.when(edge)
    def _():
        weight = weights(high * group)

        def build(h, first, count, q):
            def strip(t, q):
                rows = pl.ds(pl.multiple_of(first + t * 8, 8), 8)
                for c in range(width // 128):
                    lanes = slice(c * 128, (c + 1) * 128)
                    total = mix(weight, [2 * k + h for k in range(group)], rows, lanes)
                    node[h, rows, lanes] = total
                    q = q + total * total
                return q
            return lax.fori_loop(0, count // 8, strip, q)

        q = zero
        for k in range(pieces):
            q = build(1, k * tall, tall, q)
            node_copy(k).start()
        q = build(0, 0, block, q)
        s = zero
        for k in range(pieces):
            node_copy(k).wait_recv()

            def inner(t, s):
                rows = pl.ds(pl.multiple_of(k * tall + t * 8, 8), 8)
                for c in range(width // 128):
                    lanes = slice(c * 128, (c + 1) * 128)
                    s = s + node[0, rows, lanes] * arrived[rows, lanes]
                return s

            s = lax.fori_loop(0, tall // 8, inner, s)
        sums3[...] = row_of([s, (1.0 - up) * q, up * q])

    @pl.when(mid)
    def _():
        low, top = weights(0), weights(group)

        def strip(t, carry):
            rows = pl.ds(pl.multiple_of(t * 8, 8), 8)
            s, q, r = carry
            for c in range(width // 128):
                lanes = slice(c * 128, (c + 1) * 128)
                a = mix(low, range(group), rows, lanes)
                b = mix(top, range(group, 2 * group), rows, lanes)
                node[0, rows, lanes] = a
                node[1, rows, lanes] = b
                s, q, r = s + a * b, q + a * a, r + b * b
            return s, q, r

        s, q, r = lax.fori_loop(0, block // 8, strip, (zero,) * 3)
        sums3[...] = row_of([s, q, r])

    finish3, _, sent3 = gather(slots3, slot3_send, slot3_recv, slots3[dp * 2 + core])
    line = finish3(0, 4)
    s = lane_value(line, 0)
    low = jnp.broadcast_to(1.0 - s / (2.0 * (lane_value(line, 1) + epsilon)), (8, width))
    top = jnp.broadcast_to(1.0 - s / (2.0 * (lane_value(line, 2) + epsilon)), (8, width))

    def last(first, second, other):
        def strip(t, carry):
            rows = pl.ds(pl.multiple_of(t * 8, 8), 8)
            comb[rows, :] = first * node[0, rows, :] + second * other[rows, :]
            return carry
        lax.fori_loop(0, block // 8, strip, 0)

    @pl.when(edge)
    def _():
        last((1.0 - up) * low + up * top, up * low + (1.0 - up) * top, arrived)

    @pl.when(mid)
    def _():
        last(low, top, node.at[1])

    @pl.when(edge)
    def _():
        settled(far_edge_z, 1)

    def drained(send, ref, count):
        rows = ref.at[pl.ds(0, count)]
        pltpu.make_async_remote_copy(
            src_ref=rows, dst_ref=rows, send_sem=send, recv_sem=part_sem.at[1],
            device_id=(dp, mate), device_id_type=MESH,
        ).wait_send()

    part.wait_send()

    @pl.when(mid)
    def _():
        drained(og_send, grads, 7)
        drained(mate_send, grads, group)
        drained(act_send, acts, n_dp - 1)

    @pl.when(edge)
    def _():
        drained(og_send, grads, 4)
        drained(mate_send, grads, group // 2)
        drained(act_send, acts, n_dp - 2)
        node_sent = pltpu.make_async_remote_copy(
            src_ref=node.at[1], dst_ref=arrived, send_sem=node_send, recv_sem=node_recv.at[0],
            device_id=(far, core), device_id_type=MESH,
        )
        node_sent.wait_send()

    sent()
    sent3()


ORDER = (3, 1, 0, 2)
BATCHES = (
    (
        ((3, 4),),
        (
            (3, 5), (3, 6), (3, 7), (2, 4), (2, 5), (2, 6), (2, 7),
            (0, 3), (0, 2), (0, 1), (1, 3), (1, 2), (1, 1),
        ),
    ),
    (
        ((3, 4), (0, 4)),
        (
            (3, 5), (0, 5), (3, 6), (0, 6), (3, 7), (0, 7), (1, 4), (1, 5), (1, 6), (1, 7),
            (2, 3), (2, 2), (2, 1),
        ),
    ),
)


def exchange(n_dp, pre_act, out_weight, out_grad):
    tokens, hidden = pre_act.shape
    block = hidden // n_dp
    width = out_grad.shape[1]
    own_rows = out_grad.shape[0]
    step_cols = hidden // 8
    pieces = 4
    dma = pltpu.SemaphoreType.DMA
    hbm = pl.BlockSpec(memory_space=pl.ANY)
    vmem = pl.BlockSpec(memory_space=pltpu.VMEM)
    return pl.pallas_call(
        functools.partial(kernel, n_dp),
        out_shape=(
            jax.ShapeDtypeStruct((own_rows, width), jnp.bfloat16),
            jax.ShapeDtypeStruct((block, width), jnp.float32),
        ),
        in_specs=[hbm, hbm, hbm],
        out_specs=(vmem, vmem),
        scratch_shapes=[
            pltpu.VMEM((n_dp, tokens, block), jnp.bfloat16),
            pltpu.VMEM((n_dp, tokens, width), jnp.bfloat16),
            pltpu.VMEM((n_dp, block, width), jnp.float32),
            pltpu.VMEM((2, block, width), jnp.float32),
            pltpu.VMEM((block, width), jnp.float32),
            pltpu.VMEM((2, tokens, step_cols), jnp.bfloat16),
            pltpu.VMEM((2, step_cols, width), jnp.bfloat16),
            pltpu.VMEM((tokens, width), jnp.float32),
            pltpu.VMEM((own_rows, width), jnp.float32),
            pltpu.VMEM((128, 128), jnp.float32),
            pltpu.VMEM((2 * n_dp, 1, 128), jnp.float32),
            pltpu.VMEM((2 * n_dp, 1, 128), jnp.float32),
            pltpu.VMEM((n_dp, 128), jnp.float32),
            dma, dma((n_dp,)), dma, dma((n_dp,)), dma, dma((n_dp,)), dma,
            dma((2, 2)), dma((2,)), dma, dma((4,)), dma, dma((pieces,)), dma, dma((4,)),
            pltpu.SemaphoreType.REGULAR((6,)),
        ],
        compiler_params=pltpu.CompilerParams(
            collective_id=0, has_side_effects=True, vmem_limit_bytes=52 * 2**20
        ),
    )(pre_act, out_weight, out_grad)


def local(pre_act, out_weight, out_grad):
    n_dp = lax.axis_size("dp")
    block = pre_act.shape[1] // n_dp
    rows = out_grad.shape[0]
    if lax.axis_size("mp") == 2 and n_dp == 4 * len(ORDER) and block % 128 == 0 and rows % 16 == 0:
        return exchange(n_dp, pre_act, out_weight, out_grad)
    return halving(pre_act, out_weight, out_grad)


def solution(mesh):
    placed = (P("dp", "mp"), P("mp", None), P(("dp", "mp"), None))
    return jax.shard_map(
        local,
        mesh=mesh,
        in_specs=placed,
        out_specs=(P(("dp", "mp"), None), P(("mp", "dp"), None)),
        check_vma=False,
    )
```

```python
import functools
import jax
import jax.numpy as jnp
from jax import lax
from jax.experimental import pallas as pl
from jax.experimental.pallas import tpu as pltpu
from jax.sharding import PartitionSpec as P

epsilon = 1e-06
MESH = pl.DeviceIdType.MESH


def from_partner(value, axis, apart):
    mask = 2**apart
    pairs = [(source, source ^ mask) for source in range(lax.axis_size(axis))]
    return lax.ppermute(value, axis, pairs)


def contract(left, right):
    return lax.dot_general(
        left, right, (((0,), (0,)), ((), ())), preferred_element_type=jnp.float32
    )


def split_rows(piece, block, which):
    width = piece.shape[1]
    blocks = piece.reshape(piece.shape[0] // (2 * block), 2, block, width)
    kept = lax.dynamic_index_in_dim(blocks, which, 1, False).reshape(-1, width)
    sent = lax.dynamic_index_in_dim(blocks, 1 - which, 1, False).reshape(-1, width)
    return (kept, sent)


def level_sums(partial_value, level):
    totals = lax.psum(partial_value, "mp")
    for inner_bit in range(level + 1):
        totals = totals + from_partner(totals, "dp", inner_bit)
    return totals


def merge_level(own, other, level, which):
    lower = which == 0
    own_sq = jnp.sum(own * own)
    other_sq = jnp.sum(other * other)
    partial_value = jnp.stack(
        [
            jnp.sum(own * other),
            jnp.where(lower, own_sq, other_sq),
            jnp.where(lower, other_sq, own_sq),
        ]
    )
    totals = level_sums(partial_value, level)
    first_coef = 1.0 - totals[0] / (2.0 * (totals[1] + epsilon))
    second_coef = 1.0 - totals[0] / (2.0 * (totals[2] + epsilon))
    own_coef = jnp.where(lower, first_coef, second_coef)
    other_coef = jnp.where(lower, second_coef, first_coef)
    return own_coef * own + other_coef * other


def halving(pre_act, out_weight, out_grad):
    act = jnp.maximum(pre_act, jnp.zeros((), jnp.bfloat16))
    tokens = act.shape[0]
    partial_out = jnp.dot(act, out_weight, preferred_element_type=jnp.float32)
    summed = lax.psum_scatter(partial_out, "mp", scatter_dimension=0, tiled=True)
    projected = summed.astype(jnp.bfloat16)
    grad_full = lax.all_gather(out_grad, "mp", axis=0, tiled=True)
    count = lax.axis_size("dp")
    levels = count.bit_length() - 1
    me = lax.axis_index("dp")
    block = act.shape[1] // count
    first_bit = me & 1
    groups = act.reshape(tokens, act.shape[1] // (2 * block), 2, block)
    kept_act = lax.dynamic_index_in_dim(groups, first_bit, 2, False).reshape(tokens, -1)
    sent_act = lax.dynamic_index_in_dim(groups, 1 - first_bit, 2, False).reshape(tokens, -1)
    packed = jnp.concatenate([sent_act, grad_full], axis=1)
    arrived = from_partner(packed, "dp", 0)
    half = sent_act.shape[1]
    own = contract(kept_act, grad_full)
    other = contract(arrived[:, :half], arrived[:, half:])
    piece = merge_level(own, other, 0, first_bit)
    for level in range(1, levels):
        which = me >> level & 1
        own, sent = split_rows(piece, block, which)
        other = from_partner(sent, "dp", level)
        piece = merge_level(own, other, level, which)
    return (projected, piece)


def row_of(values):
    parts = [jnp.sum(v, axis=0, keepdims=True) for v in values]
    parts += [jnp.zeros_like(parts[0])] * (8 - len(parts))
    table = jnp.concatenate(parts, axis=0)
    return line_of(table)


def line_of(table):
    totals = jnp.sum(table, axis=1, keepdims=True)
    lane = lax.broadcasted_iota(jnp.int32, table.shape, 1)
    row = lax.broadcasted_iota(jnp.int32, table.shape, 0)
    return jnp.sum(jnp.where(lane == row, totals, 0.0), axis=0, keepdims=True)


def lane_value(line, p):
    lane = lax.broadcasted_iota(jnp.int32, line.shape, 1)
    return jnp.sum(jnp.where(lane == p, line, 0.0), axis=1, keepdims=True)


def swap(value, axis, bit):
    size = value.shape[axis]
    at = lax.broadcasted_iota(jnp.int32, value.shape, axis)
    up = pltpu.roll(value, size - bit, axis)
    down = pltpu.roll(value, bit, axis)
    return jnp.where((at // bit) % 2 == 0, up, down)


def tree_coefs(line, group):
    rows = 2 * group
    lanes = line.shape[1]
    m = jnp.concatenate([pltpu.roll(jnp.broadcast_to(line, (8, lanes)), group * r, 1)[0:1] if r else line for r in range(rows)], axis=0)
    lane = lax.broadcasted_iota(jnp.int32, m.shape, 1)
    own = lax.broadcasted_iota(jnp.int32, m.shape, 0) % group
    coef = jnp.ones_like(m)
    for level in range(group.bit_length() - 1):
        bit = 2**level
        mate = jnp.where((own // bit) % 2 == 0, own + bit, own - bit)
        inner = jnp.sum(jnp.where(lane == mate, m, 0.0), axis=1, keepdims=True)
        square = jnp.sum(jnp.where(lane == own, m, 0.0), axis=1, keepdims=True)
        f = 1.0 - inner / (2.0 * (jnp.maximum(square, 0.0) + epsilon))
        f = jnp.broadcast_to(f, m.shape)
        coef = coef * f
        across = jnp.where(lane == own, f, 0.0)
        across = jnp.concatenate(
            [jnp.broadcast_to(jnp.sum(across[g * group:(g + 1) * group], axis=0, keepdims=True), (group, lanes)) for g in range(2)],
            axis=0,
        )
        m = m * f * across
        m = m + swap(m, 1, bit)
        m = m + swap(m, 0, bit)
    return coef


def kernel(
    n_dp, pre, w, og, proj, comb,
    acts, grads, leaf, node, arrived, xbuf, wbuf, acc, part_in, gsum, slots, slots3, coefs,
    act_send, act_recv, og_send, og_recv, mate_send, mate_recv, local_sem,
    fwd_sem, part_sem, slot_send, slot_recv, node_send, node_recv, slot3_send, slot3_recv, ready,
):
    dp = lax.axis_index("dp")
    core = lax.axis_index("mp")
    group = n_dp // 2
    me = lax.rem(dp, group)
    z = dp // 4
    y = lax.rem(dp // 2, 2)
    x = lax.rem(dp, 2)
    high = z // 2
    zi = 2 * high + 1 - lax.rem(z, 2)
    tokens = pre.shape[0]
    block = pre.shape[1] // n_dp
    own_rows = og.shape[0]
    width = og.shape[1]
    mate = 1 - core
    edge_z, mid_z = 3 * high, 1 + high
    far_edge_z, far_mid_z = 3 - 3 * high, 2 - high
    edge = z == edge_z
    mid = z == mid_z

    def spot(at_z, m):
        dx = lax.rem(m, 2) if not isinstance(m, int) else m % 2
        dy = m // 2
        return at_z * 4 + (y + dy - 2 * dy * y) * 2 + x + dx - 2 * dx * x

    def turn(j):
        k = core * (ORDER[(j + 2) % 4] - ORDER[j]) + ORDER[j]
        return k

    barrier = pltpu.get_barrier_semaphore()

    def greet(sem, to, side):
        pl.semaphore_signal(sem, inc=1, device_id=(to, side), device_id_type=MESH)

    beside, behind, above, across = spot(z, 1), spot(z, 2), spot(zi, 0), spot(far_mid_z, 0)
    for to in (beside, behind, above):
        greet(barrier, to, core)
    greet(barrier, dp, mate)

    @pl.when(mid)
    def _():
        greet(barrier, across, core)

    def half(i, side):
        return grads.at[i, pl.ds(side * own_rows, own_rows)]

    home = dp
    og_local = pltpu.make_async_copy(og, half(dp, core), local_sem)
    og_local.start()

    def cols(b):
        return pl.ds(pl.multiple_of(b * block, block), block)

    def self_copy(b, slot):
        return pltpu.make_async_copy(pre.at[:, cols(b)], acts.at[slot], act_recv.at[slot])

    step_cols = xbuf.shape[2]
    steps = pre.shape[1] // step_cols

    def fetch(k, slot):
        here = pl.ds(pl.multiple_of(k * step_cols, step_cols), step_cols)
        return (
            pltpu.make_async_copy(pre.at[:, here], xbuf.at[slot], fwd_sem.at[slot, 0]),
            pltpu.make_async_copy(w.at[here, :], wbuf.at[slot], fwd_sem.at[slot, 1]),
        )

    for c in fetch(0, 0):
        c.start()
    acc[...] = jnp.zeros_like(acc)
    gsum[...] = jnp.zeros_like(gsum)

    def og_copy(n, i, to):
        return pltpu.make_async_remote_copy(
            src_ref=og if i is home else half(i, core), dst_ref=half(i, core), send_sem=og_send,
            recv_sem=og_recv.at[i], device_id=(to, core), device_id_type=MESH,
        )

    def mate_copy(i, side):
        return pltpu.make_async_remote_copy(
            src_ref=half(i, side), dst_ref=half(i, side), send_sem=mate_send,
            recv_sem=mate_recv.at[i], device_id=(dp, mate), device_id_type=MESH,
        )

    def og_arrival(i):
        og_copy(0, i, dp).wait_recv()
        mate_copy(i, core).start()

    def act_copy(kind, m):
        if kind < 2:
            to = spot(edge_z, m)
            b, slot = (to if kind == 0 else spot(far_edge_z, m)), me * 2 + kind
        else:
            to = spot(mid_z if kind == 2 else far_mid_z, m)
            b, slot = to, dp
        return pltpu.make_async_remote_copy(
            src_ref=pre.at[:, cols(b)], dst_ref=acts.at[slot],
            send_sem=act_send, recv_sem=act_recv.at[slot],
            device_id=(to, core), device_id_type=MESH,
        )

    def plan(batch, where):
        return [(kind, turn(m - 4) if m > 3 else m) for kind, m in BATCHES[where][batch]]

    def send_acts(batch):
        for where, here in ((0, edge), (1, mid)):
            @pl.when(here)
            def _():
                for kind, m in plan(batch, where):
                    act_copy(kind, m).start()

    def meet(n, to, side):
        greet(ready.at[n], to, side)
        pl.semaphore_wait(ready.at[n], 1)

    common = (
        ((z, 0, zi, 0), (z, 0, z, 1), (z, 0, z, 2), (z, 0, far_mid_z, 0), (z, 0, z, 3)),
        ((z, 1, zi, 0), (z, 2, zi, 0), (z, 3, zi, 0)),
    )
    extra = (
        (),
        (
            (z, 1, far_mid_z, 0), (z, 2, far_mid_z, 0), (z, 3, far_mid_z, 0),
            (far_edge_z, 0, z, 3), (far_edge_z, 0, z, 1), (far_edge_z, 0, z, 2),
        ),
    )
    landed = (
        ((), ()),
        (((z, 1), (z, 2), (z, 3), (zi, 0)), ((far_mid_z, 0), (far_edge_z, 0))),
        (
            ((zi, 1), (zi, 2), (zi, 3)),
            tuple((far_mid_z, m) for m in (1, 2, 3)) + tuple((far_edge_z, m) for m in (1, 2, 3)),
        ),
    )

    def og_wave(k, moves):
        base = sum(len(c) for c in moves[:k])
        base += sum(len(c) for c in common) if moves is extra else 0
        return [og_copy(base + n, home if a is z and m == 0 else spot(a, m), spot(b, r)) for n, (a, m, b, r) in enumerate(moves[k])]

    def wave(k):
        for i in landed[k][0]:
            og_arrival(spot(*i))

        @pl.when(mid)
        def _():
            for i in landed[k][1]:
                og_arrival(spot(*i))

        if k < len(common):
            for c in og_wave(k, common):
                c.start()

            @pl.when(mid)
            def _():
                for c in og_wave(k, extra):
                    c.start()

            send_acts(k)

    first = og_wave(0, common)

    @pl.when(edge)
    def _():
        pl.semaphore_wait(barrier, 4)

    @pl.when(mid)
    def _():
        pl.semaphore_wait(barrier, 5)
        first[3].start()

    for c in first[:3]:
        c.start()
    og_local.wait()
    mate_copy(dp, core).start()
    meet(0, above, core)

    @pl.when(edge)
    def _():
        first[3].start()

    meet(1, beside, core)
    meet(2, behind, core)
    first[4].start()
    send_acts(0)

    @pl.when(edge)
    def _():
        self_copy(dp, me * 2).start()
        self_copy(spot(far_edge_z, 0), me * 2 + 1).start()

    @pl.when(mid)
    def _():
        self_copy(dp, dp).start()

    def forward(k, carry):
        slot = lax.rem(k, 2)

        @pl.when(k + 1 < steps)
        def _():
            for c in fetch(k + 1, 1 - slot):
                c.start()

        for c in fetch(k, slot):
            c.wait()
        v = jnp.maximum(xbuf[slot], jnp.zeros((), jnp.bfloat16))
        acc[...] += jnp.dot(v, wbuf[slot], preferred_element_type=jnp.float32)
        return carry

    lax.fori_loop(0, steps, forward, 0)
    part = pltpu.make_async_remote_copy(
        src_ref=acc.at[pl.ds(mate * own_rows, own_rows)], dst_ref=part_in,
        send_sem=part_sem.at[0], recv_sem=part_sem.at[1],
        device_id=(dp, mate), device_id_type=MESH,
    )
    part.start()
    wave(1)
    meet(3, dp, mate)

    @pl.when(mid)
    def _():
        meet(4, across, core)

    meet(5, above, core)
    part.wait_recv()
    proj[...] = (acc[pl.ds(core * own_rows, own_rows), :] + part_in[...]).astype(proj.dtype)
    wave(2)

    def settle(i):
        mate_copy(i, mate).wait_recv()

    def leaf_grad(i, slot, own):
        if own:
            self_copy(0, slot).wait()
        else:
            pltpu.make_async_remote_copy(
                src_ref=pre.at[:, cols(0)], dst_ref=acts.at[slot], send_sem=act_send,
                recv_sem=act_recv.at[slot], device_id=(dp, mate), device_id_type=MESH,
            ).wait_recv()
        a = jnp.maximum(acts[slot], jnp.zeros((), jnp.bfloat16))
        leaf[slot] = contract(a, grads[i])

    def gram(new, others):
        i, slot = new
        seen = others + [new]

        def strip(t, carry):
            for n in range(width // 128 * 4):
                rows = pl.ds(pl.multiple_of(t * 32 + n % 4 * 8, 8), 8)
                lanes = slice(n // 4 * 128, (n // 4 + 1) * 128)
                v = leaf[slot, rows, lanes]
                carry = tuple(s + v * leaf[o, rows, lanes] for s, (_, o) in zip(carry, seen[:-1])) + (carry[-1] + v * v,)
            return carry

        zero = jnp.zeros((8, 128), jnp.float32)
        sums = lax.fori_loop(0, block // 32, strip, (zero,) * len(seen))
        for s, (j, _) in zip(sums, seen):
            line = jnp.sum(s, axis=0, keepdims=True)
            for p, q in ((i, j), (j, i))[: 1 if j is i else 2]:
                at = pl.ds(lax.rem(2 * group - p, 2 * group) * group + lax.rem(q, group), 1)
                gsum[at, :] += line

    @pl.when(edge)
    def _():
        def both(h, carry):
            done = []
            for n, (at_z, m) in enumerate([(z, 0), (z, 3), (z, 2), (z, 1)] + [(zi, turn(j)) for j in range(4)]):
                i = spot(at_z, m)

                @pl.when(h == 0)
                def _():
                    settle(i)

                slot = lax.rem(i, group) * 2 + h
                leaf_grad(i, slot, n == 0)
                gram((i, slot), done)
                done = done + [(i, slot)]
            return carry

        lax.fori_loop(0, 2, both, 0)

    @pl.when(mid)
    def _():
        near, away = [], []

        def take(i, seen):
            settle(i)
            leaf_grad(i, i, i is home)
            gram((i, i), seen)
            seen.append((i, i))

        take(home, near)
        for m in (3, 2, 1):
            take(spot(z, m), near)
        for j in range(4):
            take(spot(far_edge_z, turn(j)), away)
        for j in range(4):
            take(spot(far_mid_z, turn(j)), away)
            take(spot(zi, turn(j)), near)

    plane = n_dp // 2

    def gather(buf, send, recv, line):
        mine = dp * 2 + core
        buf[mine] = line

        def copy(other, at):
            return pltpu.make_async_remote_copy(
                src_ref=buf.at[at], dst_ref=buf.at[at], send_sem=send, recv_sem=recv.at[at // plane],
                device_id=(other // 2, lax.rem(other, 2)), device_id_type=MESH,
            )

        def go(q, carry):
            copy(lax.rem(mine + q, 2 * n_dp), mine).start()
            return carry

        def landing(at_z, rows):
            here = buf.at[pl.ds(0, rows)]
            return pltpu.make_async_remote_copy(
                src_ref=here, dst_ref=here, send_sem=send, recv_sem=recv.at[at_z],
                device_id=(dp, mate), device_id_type=MESH,
            )

        def settled(first, count):
            for k in range(count):
                at_z = first + k

                @pl.when(at_z == z)
                def _():
                    landing(at_z, plane - 1).wait_recv()

                @pl.when(at_z != z)
                def _():
                    landing(at_z, plane).wait_recv()

        def finish(first, count):
            settled(first, count)
            total = buf[first * plane]
            for k in range(1, count * plane):
                total = total + buf[first * plane + k]
            return total

        lax.fori_loop(n_dp, 2 * n_dp, go, 0)
        lax.fori_loop(1, n_dp, go, 0)
        return finish, settled, landing(0, 2 * n_dp - 1).wait_send

    finish, settled, sent = gather(slots, slot_send, slot_recv, line_of(gsum[...]))

    @pl.when(edge)
    def _():
        coefs[...] = tree_coefs(finish(high, 3), group)

    @pl.when(mid)
    def _():
        coefs[...] = tree_coefs(finish(0, 4), group)

    def weights(first):
        return [jnp.broadcast_to(coefs[pl.ds(first + k, 1), :], (8, 128)) for k in range(group)]

    pieces = node_recv.shape[0]
    tall = block // pieces

    def mix(weight, places, rows, lanes):
        total = weight[0] * leaf[places[0], rows, lanes]
        for k in range(1, group):
            total = total + weight[k] * leaf[places[k], rows, lanes]
        return total

    zero = jnp.zeros((8, 128), jnp.float32)
    far = spot(far_edge_z, 0)

    def node_copy(k):
        rows = pl.ds(k * tall, tall)
        return pltpu.make_async_remote_copy(
            src_ref=node.at[1, rows], dst_ref=arrived.at[rows],
            send_sem=node_send, recv_sem=node_recv.at[k],
            device_id=(far, core), device_id_type=MESH,
        )

    sums3 = slots3.at[dp * 2 + core]
    up = high.astype(jnp.float32)

    @pl.when(edge)
    def _():
        weight = weights(high * group)

        def build(h, first, count, q):
            def strip(t, q):
                rows = pl.ds(pl.multiple_of(first + t * 8, 8), 8)
                for c in range(width // 128):
                    lanes = slice(c * 128, (c + 1) * 128)
                    total = mix(weight, [2 * k + h for k in range(group)], rows, lanes)
                    node[h, rows, lanes] = total
                    q = q + total * total
                return q
            return lax.fori_loop(0, count // 8, strip, q)

        q = zero
        for k in range(pieces):
            q = build(1, k * tall, tall, q)
            node_copy(k).start()
        q = build(0, 0, block, q)
        s = zero
        for k in range(pieces):
            node_copy(k).wait_recv()

            def inner(t, s):
                rows = pl.ds(pl.multiple_of(k * tall + t * 8, 8), 8)
                for c in range(width // 128):
                    lanes = slice(c * 128, (c + 1) * 128)
                    s = s + node[0, rows, lanes] * arrived[rows, lanes]
                return s

            s = lax.fori_loop(0, tall // 8, inner, s)
        sums3[...] = row_of([s, (1.0 - up) * q, up * q])

    @pl.when(mid)
    def _():
        low, top = weights(0), weights(group)

        def strip(t, carry):
            rows = pl.ds(pl.multiple_of(t * 8, 8), 8)
            s, q, r = carry
            for c in range(width // 128):
                lanes = slice(c * 128, (c + 1) * 128)
                a = mix(low, range(group), rows, lanes)
                b = mix(top, range(group, 2 * group), rows, lanes)
                node[0, rows, lanes] = a
                node[1, rows, lanes] = b
                s, q, r = s + a * b, q + a * a, r + b * b
            return s, q, r

        s, q, r = lax.fori_loop(0, block // 8, strip, (zero,) * 3)
        sums3[...] = row_of([s, q, r])

    finish3, _, sent3 = gather(slots3, slot3_send, slot3_recv, slots3[dp * 2 + core])
    line = finish3(0, 4)
    s = lane_value(line, 0)
    low = jnp.broadcast_to(1.0 - s / (2.0 * (lane_value(line, 1) + epsilon)), (8, width))
    top = jnp.broadcast_to(1.0 - s / (2.0 * (lane_value(line, 2) + epsilon)), (8, width))

    def last(first, second, other):
        def strip(t, carry):
            rows = pl.ds(pl.multiple_of(t * 8, 8), 8)
            comb[rows, :] = first * node[0, rows, :] + second * other[rows, :]
            return carry
        lax.fori_loop(0, block // 8, strip, 0)

    @pl.when(edge)
    def _():
        last((1.0 - up) * low + up * top, up * low + (1.0 - up) * top, arrived)

    @pl.when(mid)
    def _():
        last(low, top, node.at[1])

    @pl.when(edge)
    def _():
        settled(far_edge_z, 1)

    def drained(send, ref, count):
        rows = ref.at[pl.ds(0, count)]
        pltpu.make_async_remote_copy(
            src_ref=rows, dst_ref=rows, send_sem=send, recv_sem=part_sem.at[1],
            device_id=(dp, mate), device_id_type=MESH,
        ).wait_send()

    part.wait_send()

    @pl.when(mid)
    def _():
        drained(og_send, grads, 7)
        drained(mate_send, grads, group)
        drained(act_send, acts, n_dp - 1)

    @pl.when(edge)
    def _():
        drained(og_send, grads, 4)
        drained(mate_send, grads, group // 2)
        drained(act_send, acts, n_dp - 2)
        node_sent = pltpu.make_async_remote_copy(
            src_ref=node.at[1], dst_ref=arrived, send_sem=node_send, recv_sem=node_recv.at[0],
            device_id=(far, core), device_id_type=MESH,
        )
        node_sent.wait_send()

    sent()
    sent3()


ORDER = (3, 1, 0, 2)
BATCHES = (
    (
        ((3, 4),),
        (
            (2, 4), (3, 5), (2, 5), (3, 6), (2, 6), (3, 7), (2, 7),
            (0, 3), (0, 2), (0, 1), (1, 3), (1, 2), (1, 1),
        ),
    ),
    (
        ((3, 4), (0, 4)),
        (
            (3, 5), (0, 5), (3, 6), (0, 6), (3, 7), (0, 7), (1, 4), (1, 5), (1, 6), (1, 7),
            (2, 3), (2, 2), (2, 1),
        ),
    ),
)


def exchange(n_dp, pre_act, out_weight, out_grad):
    tokens, hidden = pre_act.shape
    block = hidden // n_dp
    width = out_grad.shape[1]
    own_rows = out_grad.shape[0]
    step_cols = hidden // 8
    pieces = 4
    dma = pltpu.SemaphoreType.DMA
    hbm = pl.BlockSpec(memory_space=pl.ANY)
    vmem = pl.BlockSpec(memory_space=pltpu.VMEM)
    return pl.pallas_call(
        functools.partial(kernel, n_dp),
        out_shape=(
            jax.ShapeDtypeStruct((own_rows, width), jnp.bfloat16),
            jax.ShapeDtypeStruct((block, width), jnp.float32),
        ),
        in_specs=[hbm, hbm, pl.BlockSpec(memory_space=pltpu.HBM)],
        out_specs=(vmem, vmem),
        scratch_shapes=[
            pltpu.VMEM((n_dp, tokens, block), jnp.bfloat16),
            pltpu.VMEM((n_dp, tokens, width), jnp.bfloat16),
            pltpu.VMEM((n_dp, block, width), jnp.float32),
            pltpu.VMEM((2, block, width), jnp.float32),
            pltpu.VMEM((block, width), jnp.float32),
            pltpu.VMEM((2, tokens, step_cols), jnp.bfloat16),
            pltpu.VMEM((2, step_cols, width), jnp.bfloat16),
            pltpu.VMEM((tokens, width), jnp.float32),
            pltpu.VMEM((own_rows, width), jnp.float32),
            pltpu.VMEM((128, 128), jnp.float32),
            pltpu.VMEM((2 * n_dp, 1, 128), jnp.float32),
            pltpu.VMEM((2 * n_dp, 1, 128), jnp.float32),
            pltpu.VMEM((n_dp, 128), jnp.float32),
            dma, dma((n_dp,)), dma, dma((n_dp,)), dma, dma((n_dp,)), dma,
            dma((2, 2)), dma((2,)), dma, dma((4,)), dma, dma((pieces,)), dma, dma((4,)),
            pltpu.SemaphoreType.REGULAR((6,)),
        ],
        compiler_params=pltpu.CompilerParams(
            collective_id=0, has_side_effects=True, vmem_limit_bytes=52 * 2**20
        ),
    )(pre_act, out_weight, out_grad)


def local(pre_act, out_weight, out_grad):
    n_dp = lax.axis_size("dp")
    block = pre_act.shape[1] // n_dp
    rows = out_grad.shape[0]
    if lax.axis_size("mp") == 2 and n_dp == 4 * len(ORDER) and block % 128 == 0 and rows % 16 == 0:
        return exchange(n_dp, pre_act, out_weight, out_grad)
    return halving(pre_act, out_weight, out_grad)


def solution(mesh):
    placed = (P("dp", "mp"), P("mp", None), P(("dp", "mp"), None))
    return jax.shard_map(
        local,
        mesh=mesh,
        in_specs=placed,
        out_specs=(P(("dp", "mp"), None), P(("mp", "dp"), None)),
        check_vma=False,
    )
```

```python
import functools
import jax
import jax.numpy as jnp
from jax import lax
from jax.experimental import pallas as pl
from jax.experimental.pallas import tpu as pltpu
from jax.sharding import PartitionSpec as P

epsilon = 1e-06
MESH = pl.DeviceIdType.MESH


def from_partner(value, axis, apart):
    mask = 2**apart
    pairs = [(source, source ^ mask) for source in range(lax.axis_size(axis))]
    return lax.ppermute(value, axis, pairs)


def contract(left, right):
    return lax.dot_general(
        left, right, (((0,), (0,)), ((), ())), preferred_element_type=jnp.float32
    )


def split_rows(piece, block, which):
    width = piece.shape[1]
    blocks = piece.reshape(piece.shape[0] // (2 * block), 2, block, width)
    kept = lax.dynamic_index_in_dim(blocks, which, 1, False).reshape(-1, width)
    sent = lax.dynamic_index_in_dim(blocks, 1 - which, 1, False).reshape(-1, width)
    return (kept, sent)


def level_sums(partial_value, level):
    totals = lax.psum(partial_value, "mp")
    for inner_bit in range(level + 1):
        totals = totals + from_partner(totals, "dp", inner_bit)
    return totals


def merge_level(own, other, level, which):
    lower = which == 0
    own_sq = jnp.sum(own * own)
    other_sq = jnp.sum(other * other)
    partial_value = jnp.stack(
        [
            jnp.sum(own * other),
            jnp.where(lower, own_sq, other_sq),
            jnp.where(lower, other_sq, own_sq),
        ]
    )
    totals = level_sums(partial_value, level)
    first_coef = 1.0 - totals[0] / (2.0 * (totals[1] + epsilon))
    second_coef = 1.0 - totals[0] / (2.0 * (totals[2] + epsilon))
    own_coef = jnp.where(lower, first_coef, second_coef)
    other_coef = jnp.where(lower, second_coef, first_coef)
    return own_coef * own + other_coef * other


def halving(pre_act, out_weight, out_grad):
    act = jnp.maximum(pre_act, jnp.zeros((), jnp.bfloat16))
    tokens = act.shape[0]
    partial_out = jnp.dot(act, out_weight, preferred_element_type=jnp.float32)
    summed = lax.psum_scatter(partial_out, "mp", scatter_dimension=0, tiled=True)
    projected = summed.astype(jnp.bfloat16)
    grad_full = lax.all_gather(out_grad, "mp", axis=0, tiled=True)
    count = lax.axis_size("dp")
    levels = count.bit_length() - 1
    me = lax.axis_index("dp")
    block = act.shape[1] // count
    first_bit = me & 1
    groups = act.reshape(tokens, act.shape[1] // (2 * block), 2, block)
    kept_act = lax.dynamic_index_in_dim(groups, first_bit, 2, False).reshape(tokens, -1)
    sent_act = lax.dynamic_index_in_dim(groups, 1 - first_bit, 2, False).reshape(tokens, -1)
    packed = jnp.concatenate([sent_act, grad_full], axis=1)
    arrived = from_partner(packed, "dp", 0)
    half = sent_act.shape[1]
    own = contract(kept_act, grad_full)
    other = contract(arrived[:, :half], arrived[:, half:])
    piece = merge_level(own, other, 0, first_bit)
    for level in range(1, levels):
        which = me >> level & 1
        own, sent = split_rows(piece, block, which)
        other = from_partner(sent, "dp", level)
        piece = merge_level(own, other, level, which)
    return (projected, piece)


def row_of(values):
    parts = [jnp.sum(v, axis=0, keepdims=True) for v in values]
    parts += [jnp.zeros_like(parts[0])] * (8 - len(parts))
    table = jnp.concatenate(parts, axis=0)
    return line_of(table)


def line_of(table):
    totals = jnp.sum(table, axis=1, keepdims=True)
    lane = lax.broadcasted_iota(jnp.int32, table.shape, 1)
    row = lax.broadcasted_iota(jnp.int32, table.shape, 0)
    return jnp.sum(jnp.where(lane == row, totals, 0.0), axis=0, keepdims=True)


def lane_value(line, p):
    lane = lax.broadcasted_iota(jnp.int32, line.shape, 1)
    return jnp.sum(jnp.where(lane == p, line, 0.0), axis=1, keepdims=True)


def swap(value, axis, bit):
    size = value.shape[axis]
    at = lax.broadcasted_iota(jnp.int32, value.shape, axis)
    up = pltpu.roll(value, size - bit, axis)
    down = pltpu.roll(value, bit, axis)
    return jnp.where((at // bit) % 2 == 0, up, down)


def tree_coefs(line, group, side):
    lanes = line.shape[1]
    m = jnp.broadcast_to(line, (group, lanes))
    turned = pltpu.roll(m, group * group, 1)
    m = (turned if side else m) if isinstance(side, int) else jnp.where(side == 1, turned, m)
    lane = lax.broadcasted_iota(jnp.int32, m.shape, 1)
    own = lax.broadcasted_iota(jnp.int32, m.shape, 0)
    for level in range(group.bit_length() - 1):
        bit = 2**level
        m = jnp.where((own // bit) % 2 == 1, pltpu.roll(m, group * bit, 1), m)
    coef = jnp.ones_like(m)
    for level in range(group.bit_length() - 1):
        bit = 2**level
        mate = jnp.where((own // bit) % 2 == 0, own + bit, own - bit)
        inner = jnp.sum(jnp.where(lane == mate, m, 0.0), axis=1, keepdims=True)
        square = jnp.sum(jnp.where(lane == own, m, 0.0), axis=1, keepdims=True)
        f = 1.0 - inner / (2.0 * (jnp.maximum(square, 0.0) + epsilon))
        f = jnp.broadcast_to(f, m.shape)
        coef = coef * f
        if 2 * bit < group:
            across = jnp.sum(jnp.where(lane == own, f, 0.0), axis=0, keepdims=True)
            m = m * f * jnp.broadcast_to(across, m.shape)
            m = m + swap(m, 1, bit)
            m = m + swap(m, 0, bit)
    return coef


def kernel(
    n_dp, pre, w, og, proj, comb,
    acts, grads, leaf, node, arrived, xbuf, wbuf, acc, part_in, gsum, slots, slots3, coefs,
    act_send, act_recv, og_send, og_recv, mate_send, mate_recv, local_sem,
    fwd_sem, part_sem, slot_send, slot_recv, node_send, node_recv, slot3_send, slot3_recv, ready,
):
    dp = lax.axis_index("dp")
    core = lax.axis_index("mp")
    group = n_dp // 2
    me = lax.rem(dp, group)
    z = dp // 4
    y = lax.rem(dp // 2, 2)
    x = lax.rem(dp, 2)
    high = z // 2
    zi = 2 * high + 1 - lax.rem(z, 2)
    tokens = pre.shape[0]
    block = pre.shape[1] // n_dp
    own_rows = og.shape[0]
    width = og.shape[1]
    mate = 1 - core
    edge_z, mid_z = 3 * high, 1 + high
    far_edge_z, far_mid_z = 3 - 3 * high, 2 - high
    edge = z == edge_z
    mid = z == mid_z

    def spot(at_z, m):
        dx = lax.rem(m, 2) if not isinstance(m, int) else m % 2
        dy = m // 2
        return at_z * 4 + (y + dy - 2 * dy * y) * 2 + x + dx - 2 * dx * x

    def turn(j):
        k = core * (ORDER[(j + 2) % 4] - ORDER[j]) + ORDER[j]
        return k

    barrier = pltpu.get_barrier_semaphore()

    def greet(sem, to, side):
        pl.semaphore_signal(sem, inc=1, device_id=(to, side), device_id_type=MESH)

    beside, behind, above, across = spot(z, 1), spot(z, 2), spot(zi, 0), spot(far_mid_z, 0)
    for to in (beside, behind, above):
        greet(barrier, to, core)
    greet(barrier, dp, mate)

    @pl.when(mid)
    def _():
        greet(barrier, across, core)

    def half(i, side):
        return grads.at[i, pl.ds(side * own_rows, own_rows)]

    home = dp
    og_local = pltpu.make_async_copy(og, half(dp, core), local_sem)
    og_local.start()

    def cols(b):
        return pl.ds(pl.multiple_of(b * block, block), block)

    def self_copy(b, slot):
        return pltpu.make_async_copy(pre.at[:, cols(b)], acts.at[slot], act_recv.at[slot])

    step_cols = xbuf.shape[2]
    steps = pre.shape[1] // step_cols

    def fetch(k, slot):
        here = pl.ds(pl.multiple_of(k * step_cols, step_cols), step_cols)
        return (
            pltpu.make_async_copy(pre.at[:, here], xbuf.at[slot], fwd_sem.at[slot, 0]),
            pltpu.make_async_copy(w.at[here, :], wbuf.at[slot], fwd_sem.at[slot, 1]),
        )

    for c in fetch(0, 0):
        c.start()
    acc[...] = jnp.zeros_like(acc)
    gsum[...] = jnp.zeros_like(gsum)

    def og_copy(n, i, to):
        return pltpu.make_async_remote_copy(
            src_ref=og if i is home else half(i, core), dst_ref=half(i, core), send_sem=og_send,
            recv_sem=og_recv.at[i], device_id=(to, core), device_id_type=MESH,
        )

    def mate_copy(i, side):
        return pltpu.make_async_remote_copy(
            src_ref=half(i, side), dst_ref=half(i, side), send_sem=mate_send,
            recv_sem=mate_recv.at[i], device_id=(dp, mate), device_id_type=MESH,
        )

    def og_arrival(i):
        og_copy(0, i, dp).wait_recv()
        mate_copy(i, core).start()

    def act_copy(kind, m):
        if kind < 2:
            to = spot(edge_z, m)
            b, slot = (to if kind == 0 else spot(far_edge_z, m)), me * 2 + kind
        else:
            to = spot(mid_z if kind == 2 else far_mid_z, m)
            b, slot = to, dp
        return pltpu.make_async_remote_copy(
            src_ref=pre.at[:, cols(b)], dst_ref=acts.at[slot],
            send_sem=act_send, recv_sem=act_recv.at[slot],
            device_id=(to, core), device_id_type=MESH,
        )

    def plan(batch, where):
        return [(kind, turn(m - 4) if m > 3 else m) for kind, m in BATCHES[where][batch]]

    def send_acts(batch):
        for where, here in ((0, edge), (1, mid)):
            @pl.when(here)
            def _():
                for kind, m in plan(batch, where):
                    act_copy(kind, m).start()

    def meet(n, to, side):
        greet(ready.at[n], to, side)
        pl.semaphore_wait(ready.at[n], 1)

    common = (
        ((z, 0, zi, 0), (z, 0, z, 1), (z, 0, z, 2), (z, 0, far_mid_z, 0), (z, 0, z, 3)),
        ((z, 1, zi, 0), (z, 2, zi, 0), (z, 3, zi, 0)),
    )
    extra = (
        (),
        (
            (z, 1, far_mid_z, 0), (z, 2, far_mid_z, 0), (z, 3, far_mid_z, 0),
            (far_edge_z, 0, z, 3), (far_edge_z, 0, z, 1), (far_edge_z, 0, z, 2),
        ),
    )
    landed = (
        ((), ()),
        (((z, 1), (z, 2), (z, 3), (zi, 0)), ((far_mid_z, 0), (far_edge_z, 0))),
        (
            ((zi, 1), (zi, 2), (zi, 3)),
            tuple((far_mid_z, m) for m in (1, 2, 3)) + tuple((far_edge_z, m) for m in (1, 2, 3)),
        ),
    )

    def og_wave(k, moves):
        base = sum(len(c) for c in moves[:k])
        base += sum(len(c) for c in common) if moves is extra else 0
        return [og_copy(base + n, home if a is z and m == 0 else spot(a, m), spot(b, r)) for n, (a, m, b, r) in enumerate(moves[k])]

    def wave(k):
        for i in landed[k][0]:
            og_arrival(spot(*i))

        @pl.when(mid)
        def _():
            for i in landed[k][1]:
                og_arrival(spot(*i))

        if k < len(common):
            for c in og_wave(k, common):
                c.start()

            @pl.when(mid)
            def _():
                for c in og_wave(k, extra):
                    c.start()

            send_acts(k)

    first = og_wave(0, common)

    @pl.when(edge)
    def _():
        pl.semaphore_wait(barrier, 4)

    @pl.when(mid)
    def _():
        pl.semaphore_wait(barrier, 5)
        first[3].start()

    for c in first[:3]:
        c.start()
    og_local.wait()
    mate_copy(dp, core).start()
    meet(0, above, core)

    @pl.when(edge)
    def _():
        first[3].start()

    meet(1, beside, core)
    meet(2, behind, core)
    first[4].start()
    send_acts(0)

    @pl.when(edge)
    def _():
        self_copy(dp, me * 2).start()
        self_copy(spot(far_edge_z, 0), me * 2 + 1).start()

    @pl.when(mid)
    def _():
        self_copy(dp, dp).start()

    def forward(k, carry):
        slot = lax.rem(k, 2)

        @pl.when(k + 1 < steps)
        def _():
            for c in fetch(k + 1, 1 - slot):
                c.start()

        for c in fetch(k, slot):
            c.wait()
        v = jnp.maximum(xbuf[slot], jnp.zeros((), jnp.bfloat16))
        acc[...] += jnp.dot(v, wbuf[slot], preferred_element_type=jnp.float32)
        return carry

    lax.fori_loop(0, steps, forward, 0)
    part = pltpu.make_async_remote_copy(
        src_ref=acc.at[pl.ds(mate * own_rows, own_rows)], dst_ref=part_in,
        send_sem=part_sem.at[0], recv_sem=part_sem.at[1],
        device_id=(dp, mate), device_id_type=MESH,
    )
    part.start()
    wave(1)
    meet(3, dp, mate)

    @pl.when(mid)
    def _():
        meet(4, across, core)

    meet(5, above, core)
    part.wait_recv()
    proj[...] = (acc[pl.ds(core * own_rows, own_rows), :] + part_in[...]).astype(proj.dtype)

    def settle(i):
        mate_copy(i, mate).wait_recv()

    def leaf_grad(i, slot, own):
        if own:
            self_copy(0, slot).wait()
        else:
            pltpu.make_async_remote_copy(
                src_ref=pre.at[:, cols(0)], dst_ref=acts.at[slot], send_sem=act_send,
                recv_sem=act_recv.at[slot], device_id=(dp, mate), device_id_type=MESH,
            ).wait_recv()
        a = jnp.maximum(acts[slot], jnp.zeros((), jnp.bfloat16))
        leaf[slot] = contract(a, grads[i])

    def gram(new, others):
        i, slot = new
        seen = others + [new]

        def strip(t, carry):
            for n in range(width // 128 * 4):
                rows = pl.ds(pl.multiple_of(t * 32 + n % 4 * 8, 8), 8)
                lanes = slice(n // 4 * 128, (n // 4 + 1) * 128)
                v = leaf[slot, rows, lanes]
                carry = tuple(s + v * leaf[o, rows, lanes] for s, (_, o) in zip(carry, seen[:-1])) + (carry[-1] + v * v,)
            return carry

        zero = jnp.zeros((8, 128), jnp.float32)
        sums = lax.fori_loop(0, block // 32, strip, (zero,) * len(seen))
        for s, (j, _) in zip(sums, seen):
            line = jnp.sum(s, axis=0, keepdims=True)
            for p, q in ((i, j), (j, i))[: 1 if j is i else 2]:
                at = pl.ds(lax.rem(2 * group - p, 2 * group) * group + lax.rem(q, group), 1)
                gsum[at, :] += line

    @pl.when(edge)
    def _():
        def both(h, carry):
            done = []
            for n, (at_z, m) in enumerate([(z, 0), (z, 3), (z, 2), (z, 1)] + [(zi, turn(j)) for j in range(4)]):
                i = spot(at_z, m)

                @pl.when(h == 0)
                def _():
                    for late in landed[2][0] if n == 4 else ():
                        og_arrival(spot(*late))
                    settle(i)

                slot = lax.rem(i, group) * 2 + h
                leaf_grad(i, slot, n == 0)
                gram((i, slot), done)
                done = done + [(i, slot)]
            return carry

        lax.fori_loop(0, 2, both, 0)

    @pl.when(mid)
    def _():
        near, away = [], []

        def take(i, seen):
            settle(i)
            leaf_grad(i, i, i is home)
            gram((i, i), seen)
            seen.append((i, i))

        take(home, near)
        for m in (3, 2, 1):
            take(spot(z, m), near)
        for late in landed[2][0] + landed[2][1]:
            og_arrival(spot(*late))
        for j in range(4):
            take(spot(far_edge_z, turn(j)), away)
        for j in range(4):
            take(spot(far_mid_z, turn(j)), away)
            take(spot(zi, turn(j)), near)

    plane = n_dp // 2

    def gather(buf, send, recv, line):
        mine = dp * 2 + core
        buf[mine] = line

        def copy(other, at):
            return pltpu.make_async_remote_copy(
                src_ref=buf.at[at], dst_ref=buf.at[at], send_sem=send, recv_sem=recv.at[at // plane],
                device_id=(other // 2, lax.rem(other, 2)), device_id_type=MESH,
            )

        def go(q, carry):
            copy(lax.rem(mine + q, 2 * n_dp), mine).start()
            return carry

        def landing(at_z, rows):
            here = buf.at[pl.ds(0, rows)]
            return pltpu.make_async_remote_copy(
                src_ref=here, dst_ref=here, send_sem=send, recv_sem=recv.at[at_z],
                device_id=(dp, mate), device_id_type=MESH,
            )

        def settled(first, count):
            for k in range(count):
                at_z = first + k

                @pl.when(at_z == z)
                def _():
                    landing(at_z, plane - 1).wait_recv()

                @pl.when(at_z != z)
                def _():
                    landing(at_z, plane).wait_recv()

        def finish(first, count):
            settled(first, count)
            total = buf[first * plane]
            for k in range(1, count * plane):
                total = total + buf[first * plane + k]
            return total

        lax.fori_loop(n_dp, 2 * n_dp, go, 0)
        lax.fori_loop(1, n_dp, go, 0)
        return finish, settled, landing(0, 2 * n_dp - 1).wait_send

    finish, settled, sent = gather(slots, slot_send, slot_recv, line_of(gsum[...]))

    @pl.when(edge)
    def _():
        coefs[pl.ds(pl.multiple_of(high * group, group), group), :] = tree_coefs(finish(high, 3), group, high)

    @pl.when(mid)
    def _():
        total = finish(0, 4)
        for side in range(2):
            coefs[side * group:(side + 1) * group, :] = tree_coefs(total, group, side)

    def weights(first):
        return [jnp.broadcast_to(coefs[pl.ds(first + k, 1), :], (8, 128)) for k in range(group)]

    pieces = node_recv.shape[0]
    tall = block // pieces

    def mix(weight, places, rows, lanes):
        total = weight[0] * leaf[places[0], rows, lanes]
        for k in range(1, group):
            total = total + weight[k] * leaf[places[k], rows, lanes]
        return total

    zero = jnp.zeros((8, 128), jnp.float32)
    far = spot(far_edge_z, 0)

    def node_copy(k):
        rows = pl.ds(k * tall, tall)
        return pltpu.make_async_remote_copy(
            src_ref=node.at[1, rows], dst_ref=arrived.at[rows],
            send_sem=node_send, recv_sem=node_recv.at[k],
            device_id=(far, core), device_id_type=MESH,
        )

    sums3 = slots3.at[dp * 2 + core]
    up = high.astype(jnp.float32)

    @pl.when(edge)
    def _():
        weight = weights(high * group)

        def build(h, first, count, q):
            def strip(t, q):
                rows = pl.ds(pl.multiple_of(first + t * 8, 8), 8)
                for c in range(width // 128):
                    lanes = slice(c * 128, (c + 1) * 128)
                    total = mix(weight, [2 * k + h for k in range(group)], rows, lanes)
                    node[h, rows, lanes] = total
                    q = q + total * total
                return q
            return lax.fori_loop(0, count // 8, strip, q)

        q = zero
        for k in range(pieces):
            q = build(1, k * tall, tall, q)
            node_copy(k).start()
        q = build(0, 0, block, q)
        s = zero
        for k in range(pieces):
            node_copy(k).wait_recv()

            def inner(t, s):
                rows = pl.ds(pl.multiple_of(k * tall + t * 8, 8), 8)
                for c in range(width // 128):
                    lanes = slice(c * 128, (c + 1) * 128)
                    s = s + node[0, rows, lanes] * arrived[rows, lanes]
                return s

            s = lax.fori_loop(0, tall // 8, inner, s)
        sums3[...] = row_of([s, (1.0 - up) * q, up * q])

    @pl.when(mid)
    def _():
        low, top = weights(0), weights(group)

        def strip(t, carry):
            rows = pl.ds(pl.multiple_of(t * 8, 8), 8)
            s, q, r = carry
            for c in range(width // 128):
                lanes = slice(c * 128, (c + 1) * 128)
                a = mix(low, range(group), rows, lanes)
                b = mix(top, range(group, 2 * group), rows, lanes)
                node[0, rows, lanes] = a
                node[1, rows, lanes] = b
                s, q, r = s + a * b, q + a * a, r + b * b
            return s, q, r

        s, q, r = lax.fori_loop(0, block // 8, strip, (zero,) * 3)
        sums3[...] = row_of([s, q, r])

    finish3, _, sent3 = gather(slots3, slot3_send, slot3_recv, slots3[dp * 2 + core])
    line = finish3(0, 4)
    s = lane_value(line, 0)
    low = jnp.broadcast_to(1.0 - s / (2.0 * (lane_value(line, 1) + epsilon)), (8, width))
    top = jnp.broadcast_to(1.0 - s / (2.0 * (lane_value(line, 2) + epsilon)), (8, width))

    def last(first, second, other):
        def strip(t, carry):
            rows = pl.ds(pl.multiple_of(t * 8, 8), 8)
            comb[rows, :] = first * node[0, rows, :] + second * other[rows, :]
            return carry
        lax.fori_loop(0, block // 8, strip, 0)

    @pl.when(edge)
    def _():
        last((1.0 - up) * low + up * top, up * low + (1.0 - up) * top, arrived)

    @pl.when(mid)
    def _():
        last(low, top, node.at[1])

    @pl.when(edge)
    def _():
        settled(far_edge_z, 1)

    def drained(send, ref, count):
        rows = ref.at[pl.ds(0, count)]
        pltpu.make_async_remote_copy(
            src_ref=rows, dst_ref=rows, send_sem=send, recv_sem=part_sem.at[1],
            device_id=(dp, mate), device_id_type=MESH,
        ).wait_send()

    part.wait_send()

    @pl.when(mid)
    def _():
        drained(og_send, grads, 7)
        drained(mate_send, grads, group)
        drained(act_send, acts, n_dp - 1)

    @pl.when(edge)
    def _():
        drained(og_send, grads, 4)
        drained(mate_send, grads, group // 2)
        drained(act_send, acts, n_dp - 2)
        node_sent = pltpu.make_async_remote_copy(
            src_ref=node.at[1], dst_ref=arrived, send_sem=node_send, recv_sem=node_recv.at[0],
            device_id=(far, core), device_id_type=MESH,
        )
        node_sent.wait_send()

    sent()
    sent3()


ORDER = (3, 1, 0, 2)
BATCHES = (
    (
        ((3, 4),),
        (
            (2, 4), (3, 5), (2, 5), (3, 6), (2, 6), (3, 7), (2, 7),
            (0, 3), (0, 2), (0, 1), (1, 3), (1, 2), (1, 1),
        ),
    ),
    (
        ((3, 4), (0, 4)),
        (
            (3, 5), (0, 5), (3, 6), (0, 6), (3, 7), (0, 7), (1, 4), (1, 5), (1, 6), (1, 7),
            (2, 3), (2, 2), (2, 1),
        ),
    ),
)


def exchange(n_dp, pre_act, out_weight, out_grad):
    tokens, hidden = pre_act.shape
    block = hidden // n_dp
    width = out_grad.shape[1]
    own_rows = out_grad.shape[0]
    step_cols = hidden // 8
    pieces = 4
    dma = pltpu.SemaphoreType.DMA
    hbm = pl.BlockSpec(memory_space=pl.ANY)
    vmem = pl.BlockSpec(memory_space=pltpu.VMEM)
    return pl.pallas_call(
        functools.partial(kernel, n_dp),
        out_shape=(
            jax.ShapeDtypeStruct((own_rows, width), jnp.bfloat16),
            jax.ShapeDtypeStruct((block, width), jnp.float32),
        ),
        in_specs=[hbm, hbm, pl.BlockSpec(memory_space=pltpu.HBM)],
        out_specs=(vmem, vmem),
        scratch_shapes=[
            pltpu.VMEM((n_dp, tokens, block), jnp.bfloat16),
            pltpu.VMEM((n_dp, tokens, width), jnp.bfloat16),
            pltpu.VMEM((n_dp, block, width), jnp.float32),
            pltpu.VMEM((2, block, width), jnp.float32),
            pltpu.VMEM((block, width), jnp.float32),
            pltpu.VMEM((2, tokens, step_cols), jnp.bfloat16),
            pltpu.VMEM((2, step_cols, width), jnp.bfloat16),
            pltpu.VMEM((tokens, width), jnp.float32),
            pltpu.VMEM((own_rows, width), jnp.float32),
            pltpu.VMEM((128, 128), jnp.float32),
            pltpu.VMEM((2 * n_dp, 1, 128), jnp.float32),
            pltpu.VMEM((2 * n_dp, 1, 128), jnp.float32),
            pltpu.VMEM((n_dp, 128), jnp.float32),
            dma, dma((n_dp,)), dma, dma((n_dp,)), dma, dma((n_dp,)), dma,
            dma((2, 2)), dma((2,)), dma, dma((4,)), dma, dma((pieces,)), dma, dma((4,)),
            pltpu.SemaphoreType.REGULAR((6,)),
        ],
        compiler_params=pltpu.CompilerParams(
            collective_id=0, has_side_effects=True, vmem_limit_bytes=52 * 2**20
        ),
    )(pre_act, out_weight, pltpu.with_memory_space_constraint(out_grad, pltpu.HBM))


def local(pre_act, out_weight, out_grad):
    n_dp = lax.axis_size("dp")
    block = pre_act.shape[1] // n_dp
    rows = out_grad.shape[0]
    if lax.axis_size("mp") == 2 and n_dp == 4 * len(ORDER) and block % 128 == 0 and rows % 16 == 0:
        return exchange(n_dp, pre_act, out_weight, out_grad)
    return halving(pre_act, out_weight, out_grad)


def solution(mesh):
    placed = (P("dp", "mp"), P("mp", None), P(("dp", "mp"), None))
    return jax.shard_map(
        local,
        mesh=mesh,
        in_specs=placed,
        out_specs=(P(("dp", "mp"), None), P(("mp", "dp"), None)),
        check_vma=False,
    )
```

```python
import functools
import jax
import jax.numpy as jnp
from jax import lax
from jax.experimental import pallas as pl
from jax.experimental.pallas import tpu as pltpu
from jax.sharding import PartitionSpec as P

epsilon = 1e-06
MESH = pl.DeviceIdType.MESH


def from_partner(value, axis, apart):
    mask = 2**apart
    pairs = [(source, source ^ mask) for source in range(lax.axis_size(axis))]
    return lax.ppermute(value, axis, pairs)


def contract(left, right):
    return lax.dot_general(
        left, right, (((0,), (0,)), ((), ())), preferred_element_type=jnp.float32
    )


def split_rows(piece, block, which):
    width = piece.shape[1]
    blocks = piece.reshape(piece.shape[0] // (2 * block), 2, block, width)
    kept = lax.dynamic_index_in_dim(blocks, which, 1, False).reshape(-1, width)
    sent = lax.dynamic_index_in_dim(blocks, 1 - which, 1, False).reshape(-1, width)
    return (kept, sent)


def level_sums(partial_value, level):
    totals = lax.psum(partial_value, "mp")
    for inner_bit in range(level + 1):
        totals = totals + from_partner(totals, "dp", inner_bit)
    return totals


def merge_level(own, other, level, which):
    lower = which == 0
    own_sq = jnp.sum(own * own)
    other_sq = jnp.sum(other * other)
    partial_value = jnp.stack(
        [
            jnp.sum(own * other),
            jnp.where(lower, own_sq, other_sq),
            jnp.where(lower, other_sq, own_sq),
        ]
    )
    totals = level_sums(partial_value, level)
    first_coef = 1.0 - totals[0] / (2.0 * (totals[1] + epsilon))
    second_coef = 1.0 - totals[0] / (2.0 * (totals[2] + epsilon))
    own_coef = jnp.where(lower, first_coef, second_coef)
    other_coef = jnp.where(lower, second_coef, first_coef)
    return own_coef * own + other_coef * other


def halving(pre_act, out_weight, out_grad):
    act = jnp.maximum(pre_act, jnp.zeros((), jnp.bfloat16))
    tokens = act.shape[0]
    partial_out = jnp.dot(act, out_weight, preferred_element_type=jnp.float32)
    summed = lax.psum_scatter(partial_out, "mp", scatter_dimension=0, tiled=True)
    projected = summed.astype(jnp.bfloat16)
    grad_full = lax.all_gather(out_grad, "mp", axis=0, tiled=True)
    count = lax.axis_size("dp")
    levels = count.bit_length() - 1
    me = lax.axis_index("dp")
    block = act.shape[1] // count
    first_bit = me & 1
    groups = act.reshape(tokens, act.shape[1] // (2 * block), 2, block)
    kept_act = lax.dynamic_index_in_dim(groups, first_bit, 2, False).reshape(tokens, -1)
    sent_act = lax.dynamic_index_in_dim(groups, 1 - first_bit, 2, False).reshape(tokens, -1)
    packed = jnp.concatenate([sent_act, grad_full], axis=1)
    arrived = from_partner(packed, "dp", 0)
    half = sent_act.shape[1]
    own = contract(kept_act, grad_full)
    other = contract(arrived[:, :half], arrived[:, half:])
    piece = merge_level(own, other, 0, first_bit)
    for level in range(1, levels):
        which = me >> level & 1
        own, sent = split_rows(piece, block, which)
        other = from_partner(sent, "dp", level)
        piece = merge_level(own, other, level, which)
    return (projected, piece)


def row_of(values):
    parts = [jnp.sum(v, axis=0, keepdims=True) for v in values]
    parts += [jnp.zeros_like(parts[0])] * (8 - len(parts))
    table = jnp.concatenate(parts, axis=0)
    return line_of(table)


def line_of(table):
    totals = jnp.sum(table, axis=1, keepdims=True)
    lane = lax.broadcasted_iota(jnp.int32, table.shape, 1)
    row = lax.broadcasted_iota(jnp.int32, table.shape, 0)
    return jnp.sum(jnp.where(lane == row, totals, 0.0), axis=0, keepdims=True)


def lane_value(line, p):
    lane = lax.broadcasted_iota(jnp.int32, line.shape, 1)
    return jnp.sum(jnp.where(lane == p, line, 0.0), axis=1, keepdims=True)


def swap(value, axis, bit):
    size = value.shape[axis]
    at = lax.broadcasted_iota(jnp.int32, value.shape, axis)
    up = pltpu.roll(value, size - bit, axis)
    down = pltpu.roll(value, bit, axis)
    return jnp.where((at // bit) % 2 == 0, up, down)


def tree_coefs(line, group, side):
    lanes = line.shape[1]
    m = jnp.broadcast_to(line, (group, lanes))
    turned = pltpu.roll(m, group * group, 1)
    m = (turned if side else m) if isinstance(side, int) else jnp.where(side == 1, turned, m)
    lane = lax.broadcasted_iota(jnp.int32, m.shape, 1)
    own = lax.broadcasted_iota(jnp.int32, m.shape, 0)
    for level in range(group.bit_length() - 1):
        bit = 2**level
        m = jnp.where((own // bit) % 2 == 1, pltpu.roll(m, group * bit, 1), m)
    coef = jnp.ones_like(m)
    for level in range(group.bit_length() - 1):
        bit = 2**level
        mate = jnp.where((own // bit) % 2 == 0, own + bit, own - bit)
        inner = jnp.sum(jnp.where(lane == mate, m, 0.0), axis=1, keepdims=True)
        square = jnp.sum(jnp.where(lane == own, m, 0.0), axis=1, keepdims=True)
        f = 1.0 - inner / (2.0 * (jnp.maximum(square, 0.0) + epsilon))
        f = jnp.broadcast_to(f, m.shape)
        coef = coef * f
        if 2 * bit < group:
            across = jnp.sum(jnp.where(lane == own, f, 0.0), axis=0, keepdims=True)
            m = m * f * jnp.broadcast_to(across, m.shape)
            m = m + swap(m, 1, bit)
            m = m + swap(m, 0, bit)
    return coef


def kernel(
    n_dp, pre, w, og, proj, comb,
    acts, grads, leaf, node, arrived, xbuf, wbuf, acc, part_in, gsum, slots, slots3, coefs,
    act_send, act_recv, og_send, og_recv, mate_send, mate_recv, local_sem,
    fwd_sem, part_sem, slot_send, slot_recv, node_send, node_recv, slot3_send, slot3_recv, ready,
):
    dp = lax.axis_index("dp")
    core = lax.axis_index("mp")
    group = n_dp // 2
    me = lax.rem(dp, group)
    z = dp // 4
    y = lax.rem(dp // 2, 2)
    x = lax.rem(dp, 2)
    high = z // 2
    zi = 2 * high + 1 - lax.rem(z, 2)
    tokens = pre.shape[0]
    block = pre.shape[1] // n_dp
    own_rows = og.shape[0]
    width = og.shape[1]
    mate = 1 - core
    edge_z, mid_z = 3 * high, 1 + high
    far_edge_z, far_mid_z = 3 - 3 * high, 2 - high
    edge = z == edge_z
    mid = z == mid_z

    def spot(at_z, m):
        dx = lax.rem(m, 2) if not isinstance(m, int) else m % 2
        dy = m // 2
        return at_z * 4 + (y + dy - 2 * dy * y) * 2 + x + dx - 2 * dx * x

    def turn(j):
        k = core * (ORDER[(j + 2) % 4] - ORDER[j]) + ORDER[j]
        return k

    barrier = pltpu.get_barrier_semaphore()

    def greet(sem, to, side):
        pl.semaphore_signal(sem, inc=1, device_id=(to, side), device_id_type=MESH)

    beside, behind, above, across = spot(z, 1), spot(z, 2), spot(zi, 0), spot(far_mid_z, 0)
    for to in (beside, behind, above):
        greet(barrier, to, core)
    greet(barrier, dp, mate)

    @pl.when(mid)
    def _():
        greet(barrier, across, core)

    def half(i, side):
        return grads.at[i, pl.ds(side * own_rows, own_rows)]

    home = dp
    og_local = pltpu.make_async_copy(og, half(dp, core), local_sem)
    og_local.start()

    def cols(b):
        return pl.ds(pl.multiple_of(b * block, block), block)

    def self_copy(b, slot):
        return pltpu.make_async_copy(pre.at[:, cols(b)], acts.at[slot], act_recv.at[slot])

    step_cols = xbuf.shape[2]
    steps = pre.shape[1] // step_cols

    def fetch(k, slot):
        here = pl.ds(pl.multiple_of(k * step_cols, step_cols), step_cols)
        return (
            pltpu.make_async_copy(pre.at[:, here], xbuf.at[slot], fwd_sem.at[slot, 0]),
            pltpu.make_async_copy(w.at[here, :], wbuf.at[slot], fwd_sem.at[slot, 1]),
        )

    for c in fetch(0, 0):
        c.start()
    acc[...] = jnp.zeros_like(acc)
    gsum[...] = jnp.zeros_like(gsum)

    def og_copy(n, i, to):
        return pltpu.make_async_remote_copy(
            src_ref=og if i is home else half(i, core), dst_ref=half(i, core), send_sem=og_send,
            recv_sem=og_recv.at[i], device_id=(to, core), device_id_type=MESH,
        )

    def mate_copy(i, side):
        return pltpu.make_async_remote_copy(
            src_ref=half(i, side), dst_ref=half(i, side), send_sem=mate_send,
            recv_sem=mate_recv.at[i], device_id=(dp, mate), device_id_type=MESH,
        )

    def og_arrival(i):
        og_copy(0, i, dp).wait_recv()
        mate_copy(i, core).start()

    def act_copy(kind, m):
        if kind < 2:
            to = spot(edge_z, m)
            b, slot = (to if kind == 0 else spot(far_edge_z, m)), me * 2 + kind
        else:
            to = spot(mid_z if kind == 2 else far_mid_z, m)
            b, slot = to, dp
        return pltpu.make_async_remote_copy(
            src_ref=pre.at[:, cols(b)], dst_ref=acts.at[slot],
            send_sem=act_send, recv_sem=act_recv.at[slot],
            device_id=(to, core), device_id_type=MESH,
        )

    def plan(batch, where):
        return [(kind, turn(m - 4) if m > 3 else m) for kind, m in BATCHES[where][batch]]

    def send_acts(batch):
        for where, here in ((0, edge), (1, mid)):
            @pl.when(here)
            def _():
                for kind, m in plan(batch, where):
                    act_copy(kind, m).start()

    def meet(n, to, side):
        greet(ready.at[n], to, side)
        pl.semaphore_wait(ready.at[n], 1)

    common = (
        ((z, 0, zi, 0), (z, 0, z, 1), (z, 0, z, 2), (z, 0, far_mid_z, 0), (z, 0, z, 3)),
        ((z, 1, zi, 0), (z, 2, zi, 0), (z, 3, zi, 0)),
    )
    extra = (
        (),
        (
            (z, 1, far_mid_z, 0), (z, 2, far_mid_z, 0), (z, 3, far_mid_z, 0),
            (far_edge_z, 0, z, 3), (far_edge_z, 0, z, 1), (far_edge_z, 0, z, 2),
        ),
    )
    landed = (
        ((), ()),
        (((z, 1), (z, 2), (z, 3), (zi, 0)), ((far_mid_z, 0), (far_edge_z, 0))),
        (
            ((zi, 1), (zi, 2), (zi, 3)),
            tuple((far_mid_z, m) for m in (1, 2, 3)) + tuple((far_edge_z, m) for m in (1, 2, 3)),
        ),
    )

    def og_wave(k, moves):
        base = sum(len(c) for c in moves[:k])
        base += sum(len(c) for c in common) if moves is extra else 0
        return [og_copy(base + n, home if a is z and m == 0 else spot(a, m), spot(b, r)) for n, (a, m, b, r) in enumerate(moves[k])]

    def wave(k):
        for i in landed[k][0]:
            og_arrival(spot(*i))

        @pl.when(mid)
        def _():
            for i in landed[k][1]:
                og_arrival(spot(*i))

        if k < len(common):
            for c in og_wave(k, common):
                c.start()

            @pl.when(mid)
            def _():
                for c in og_wave(k, extra):
                    c.start()

            send_acts(k)

    first = og_wave(0, common)

    @pl.when(edge)
    def _():
        pl.semaphore_wait(barrier, 4)

    @pl.when(mid)
    def _():
        pl.semaphore_wait(barrier, 5)
        first[3].start()

    for c in first[:3]:
        c.start()
    og_local.wait()
    mate_copy(dp, core).start()
    meet(0, above, core)

    @pl.when(edge)
    def _():
        first[3].start()

    meet(1, beside, core)
    meet(2, behind, core)
    first[4].start()
    send_acts(0)

    @pl.when(edge)
    def _():
        self_copy(dp, me * 2).start()
        self_copy(spot(far_edge_z, 0), me * 2 + 1).start()

    @pl.when(mid)
    def _():
        self_copy(dp, dp).start()

    def forward(k, carry):
        slot = lax.rem(k, 2)

        @pl.when(k + 1 < steps)
        def _():
            for c in fetch(k + 1, 1 - slot):
                c.start()

        for c in fetch(k, slot):
            c.wait()
        v = jnp.maximum(xbuf[slot], jnp.zeros((), jnp.bfloat16))
        acc[...] += jnp.dot(v, wbuf[slot], preferred_element_type=jnp.float32)
        return carry

    lax.fori_loop(0, steps // 2, forward, 0)
    wave(1)
    lax.fori_loop(steps // 2, steps, forward, 0)
    part = pltpu.make_async_remote_copy(
        src_ref=acc.at[pl.ds(mate * own_rows, own_rows)], dst_ref=part_in,
        send_sem=part_sem.at[0], recv_sem=part_sem.at[1],
        device_id=(dp, mate), device_id_type=MESH,
    )
    part.start()
    meet(3, dp, mate)

    @pl.when(mid)
    def _():
        meet(4, across, core)

    meet(5, above, core)
    part.wait_recv()
    proj[...] = (acc[pl.ds(core * own_rows, own_rows), :] + part_in[...]).astype(proj.dtype)

    def settle(i):
        mate_copy(i, mate).wait_recv()

    def leaf_grad(i, slot, own):
        if own:
            self_copy(0, slot).wait()
        else:
            pltpu.make_async_remote_copy(
                src_ref=pre.at[:, cols(0)], dst_ref=acts.at[slot], send_sem=act_send,
                recv_sem=act_recv.at[slot], device_id=(dp, mate), device_id_type=MESH,
            ).wait_recv()
        a = jnp.maximum(acts[slot], jnp.zeros((), jnp.bfloat16))
        leaf[slot] = contract(a, grads[i])

    def gram(new, others):
        i, slot = new
        seen = others + [new]

        def strip(t, carry):
            for n in range(width // 128 * 4):
                rows = pl.ds(pl.multiple_of(t * 32 + n % 4 * 8, 8), 8)
                lanes = slice(n // 4 * 128, (n // 4 + 1) * 128)
                v = leaf[slot, rows, lanes]
                carry = tuple(s + v * leaf[o, rows, lanes] for s, (_, o) in zip(carry, seen[:-1])) + (carry[-1] + v * v,)
            return carry

        zero = jnp.zeros((8, 128), jnp.float32)
        sums = lax.fori_loop(0, block // 32, strip, (zero,) * len(seen))
        for s, (j, _) in zip(sums, seen):
            line = jnp.sum(s, axis=0, keepdims=True)
            for p, q in ((i, j), (j, i))[: 1 if j is i else 2]:
                at = pl.ds(lax.rem(2 * group - p, 2 * group) * group + lax.rem(q, group), 1)
                gsum[at, :] += line

    @pl.when(edge)
    def _():
        def both(h, carry):
            done = []
            for n, (at_z, m) in enumerate([(z, 0), (z, 3), (z, 2), (z, 1)] + [(zi, turn(j)) for j in range(4)]):
                i = spot(at_z, m)

                @pl.when(h == 0)
                def _():
                    for late in landed[2][0] if n == 4 else ():
                        og_arrival(spot(*late))
                    settle(i)

                slot = lax.rem(i, group) * 2 + h
                leaf_grad(i, slot, n == 0)
                gram((i, slot), done)
                done = done + [(i, slot)]
            return carry

        lax.fori_loop(0, 2, both, 0)

    @pl.when(mid)
    def _():
        near, away = [], []

        def take(i, seen):
            settle(i)
            leaf_grad(i, i, i is home)
            gram((i, i), seen)
            seen.append((i, i))

        take(home, near)
        for m in (3, 2, 1):
            take(spot(z, m), near)
        for late in landed[2][0] + landed[2][1]:
            og_arrival(spot(*late))
        for j in range(4):
            take(spot(far_edge_z, turn(j)), away)
        for j in range(4):
            take(spot(far_mid_z, turn(j)), away)
            take(spot(zi, turn(j)), near)

    plane = n_dp // 2

    def gather(buf, send, recv, line):
        mine = dp * 2 + core
        buf[mine] = line

        def copy(other, at):
            return pltpu.make_async_remote_copy(
                src_ref=buf.at[at], dst_ref=buf.at[at], send_sem=send, recv_sem=recv.at[at // plane],
                device_id=(other // 2, lax.rem(other, 2)), device_id_type=MESH,
            )

        def go(q, carry):
            copy(lax.rem(mine + q, 2 * n_dp), mine).start()
            return carry

        def landing(at_z, rows):
            here = buf.at[pl.ds(0, rows)]
            return pltpu.make_async_remote_copy(
                src_ref=here, dst_ref=here, send_sem=send, recv_sem=recv.at[at_z],
                device_id=(dp, mate), device_id_type=MESH,
            )

        def settled(first, count):
            for k in range(count):
                at_z = first + k

                @pl.when(at_z == z)
                def _():
                    landing(at_z, plane - 1).wait_recv()

                @pl.when(at_z != z)
                def _():
                    landing(at_z, plane).wait_recv()

        def finish(first, count):
            settled(first, count)
            total = buf[first * plane]
            for k in range(1, count * plane):
                total = total + buf[first * plane + k]
            return total

        lax.fori_loop(n_dp, 2 * n_dp, go, 0)
        lax.fori_loop(1, n_dp, go, 0)
        return finish, settled, landing(0, 2 * n_dp - 1).wait_send

    finish, settled, sent = gather(slots, slot_send, slot_recv, line_of(gsum[...]))

    @pl.when(edge)
    def _():
        coefs[pl.ds(pl.multiple_of(high * group, group), group), :] = tree_coefs(finish(high, 3), group, high)

    @pl.when(mid)
    def _():
        total = finish(0, 4)
        for side in range(2):
            coefs[side * group:(side + 1) * group, :] = tree_coefs(total, group, side)

    def weights(first):
        return [jnp.broadcast_to(coefs[pl.ds(first + k, 1), :], (8, 128)) for k in range(group)]

    pieces = node_recv.shape[0]
    tall = block // pieces

    def mix(weight, places, rows, lanes):
        total = weight[0] * leaf[places[0], rows, lanes]
        for k in range(1, group):
            total = total + weight[k] * leaf[places[k], rows, lanes]
        return total

    zero = jnp.zeros((8, 128), jnp.float32)
    far = spot(far_edge_z, 0)

    def node_copy(k):
        rows = pl.ds(k * tall, tall)
        return pltpu.make_async_remote_copy(
            src_ref=node.at[1, rows], dst_ref=arrived.at[rows],
            send_sem=node_send, recv_sem=node_recv.at[k],
            device_id=(far, core), device_id_type=MESH,
        )

    sums3 = slots3.at[dp * 2 + core]
    up = high.astype(jnp.float32)

    @pl.when(edge)
    def _():
        weight = weights(high * group)

        def build(h, first, count, q):
            def strip(t, q):
                rows = pl.ds(pl.multiple_of(first + t * 8, 8), 8)
                for c in range(width // 128):
                    lanes = slice(c * 128, (c + 1) * 128)
                    total = mix(weight, [2 * k + h for k in range(group)], rows, lanes)
                    node[h, rows, lanes] = total
                    q = q + total * total
                return q
            return lax.fori_loop(0, count // 8, strip, q)

        q = zero
        for k in range(pieces):
            q = build(1, k * tall, tall, q)
            node_copy(k).start()
        q = build(0, 0, block, q)
        s = zero
        for k in range(pieces):
            node_copy(k).wait_recv()

            def inner(t, s):
                rows = pl.ds(pl.multiple_of(k * tall + t * 8, 8), 8)
                for c in range(width // 128):
                    lanes = slice(c * 128, (c + 1) * 128)
                    s = s + node[0, rows, lanes] * arrived[rows, lanes]
                return s

            s = lax.fori_loop(0, tall // 8, inner, s)
        sums3[...] = row_of([s, (1.0 - up) * q, up * q])

    @pl.when(mid)
    def _():
        low, top = weights(0), weights(group)

        def strip(t, carry):
            rows = pl.ds(pl.multiple_of(t * 8, 8), 8)
            s, q, r = carry
            for c in range(width // 128):
                lanes = slice(c * 128, (c + 1) * 128)
                a = mix(low, range(group), rows, lanes)
                b = mix(top, range(group, 2 * group), rows, lanes)
                node[0, rows, lanes] = a
                node[1, rows, lanes] = b
                s, q, r = s + a * b, q + a * a, r + b * b
            return s, q, r

        s, q, r = lax.fori_loop(0, block // 8, strip, (zero,) * 3)
        sums3[...] = row_of([s, q, r])

    finish3, _, sent3 = gather(slots3, slot3_send, slot3_recv, slots3[dp * 2 + core])
    line = finish3(0, 4)
    s = lane_value(line, 0)
    low = jnp.broadcast_to(1.0 - s / (2.0 * (lane_value(line, 1) + epsilon)), (8, width))
    top = jnp.broadcast_to(1.0 - s / (2.0 * (lane_value(line, 2) + epsilon)), (8, width))

    def last(first, second, other):
        def strip(t, carry):
            rows = pl.ds(pl.multiple_of(t * 8, 8), 8)
            comb[rows, :] = first * node[0, rows, :] + second * other[rows, :]
            return carry
        lax.fori_loop(0, block // 8, strip, 0)

    @pl.when(edge)
    def _():
        last((1.0 - up) * low + up * top, up * low + (1.0 - up) * top, arrived)

    @pl.when(mid)
    def _():
        last(low, top, node.at[1])

    @pl.when(edge)
    def _():
        settled(far_edge_z, 1)

    def drained(send, ref, count):
        rows = ref.at[pl.ds(0, count)]
        pltpu.make_async_remote_copy(
            src_ref=rows, dst_ref=rows, send_sem=send, recv_sem=part_sem.at[1],
            device_id=(dp, mate), device_id_type=MESH,
        ).wait_send()

    part.wait_send()

    @pl.when(mid)
    def _():
        drained(og_send, grads, 7)
        drained(mate_send, grads, group)
        drained(act_send, acts, n_dp - 1)

    @pl.when(edge)
    def _():
        drained(og_send, grads, 4)
        drained(mate_send, grads, group // 2)
        drained(act_send, acts, n_dp - 2)
        node_sent = pltpu.make_async_remote_copy(
            src_ref=node.at[1], dst_ref=arrived, send_sem=node_send, recv_sem=node_recv.at[0],
            device_id=(far, core), device_id_type=MESH,
        )
        node_sent.wait_send()

    sent()
    sent3()


ORDER = (3, 1, 0, 2)
BATCHES = (
    (
        ((3, 4),),
        (
            (2, 4), (3, 5), (2, 5), (3, 6), (2, 6), (3, 7), (2, 7),
            (0, 3), (0, 2), (0, 1), (1, 3), (1, 2), (1, 1),
        ),
    ),
    (
        ((3, 4), (0, 4)),
        (
            (3, 5), (0, 5), (3, 6), (0, 6), (3, 7), (0, 7), (1, 4), (1, 5), (1, 6), (1, 7),
            (2, 3), (2, 2), (2, 1),
        ),
    ),
)


def exchange(n_dp, pre_act, out_weight, out_grad):
    tokens, hidden = pre_act.shape
    block = hidden // n_dp
    width = out_grad.shape[1]
    own_rows = out_grad.shape[0]
    step_cols = hidden // 8
    pieces = 8
    dma = pltpu.SemaphoreType.DMA
    hbm = pl.BlockSpec(memory_space=pl.ANY)
    vmem = pl.BlockSpec(memory_space=pltpu.VMEM)
    return pl.pallas_call(
        functools.partial(kernel, n_dp),
        out_shape=(
            jax.ShapeDtypeStruct((own_rows, width), jnp.bfloat16),
            jax.ShapeDtypeStruct((block, width), jnp.float32),
        ),
        in_specs=[hbm, hbm, pl.BlockSpec(memory_space=pltpu.HBM)],
        out_specs=(vmem, vmem),
        scratch_shapes=[
            pltpu.VMEM((n_dp, tokens, block), jnp.bfloat16),
            pltpu.VMEM((n_dp, tokens, width), jnp.bfloat16),
            pltpu.VMEM((n_dp, block, width), jnp.float32),
            pltpu.VMEM((2, block, width), jnp.float32),
            pltpu.VMEM((block, width), jnp.float32),
            pltpu.VMEM((2, tokens, step_cols), jnp.bfloat16),
            pltpu.VMEM((2, step_cols, width), jnp.bfloat16),
            pltpu.VMEM((tokens, width), jnp.float32),
            pltpu.VMEM((own_rows, width), jnp.float32),
            pltpu.VMEM((128, 128), jnp.float32),
            pltpu.VMEM((2 * n_dp, 1, 128), jnp.float32),
            pltpu.VMEM((2 * n_dp, 1, 128), jnp.float32),
            pltpu.VMEM((n_dp, 128), jnp.float32),
            dma, dma((n_dp,)), dma, dma((n_dp,)), dma, dma((n_dp,)), dma,
            dma((2, 2)), dma((2,)), dma, dma((4,)), dma, dma((pieces,)), dma, dma((4,)),
            pltpu.SemaphoreType.REGULAR((6,)),
        ],
        compiler_params=pltpu.CompilerParams(
            collective_id=0, has_side_effects=True, vmem_limit_bytes=52 * 2**20
        ),
    )(pre_act, out_weight, pltpu.with_memory_space_constraint(out_grad, pltpu.HBM))


def local(pre_act, out_weight, out_grad):
    n_dp = lax.axis_size("dp")
    block = pre_act.shape[1] // n_dp
    rows = out_grad.shape[0]
    if lax.axis_size("mp") == 2 and n_dp == 4 * len(ORDER) and block % 128 == 0 and rows % 16 == 0:
        return exchange(n_dp, pre_act, out_weight, out_grad)
    return halving(pre_act, out_weight, out_grad)


def solution(mesh):
    placed = (P("dp", "mp"), P("mp", None), P(("dp", "mp"), None))
    return jax.shard_map(
        local,
        mesh=mesh,
        in_specs=placed,
        out_specs=(P(("dp", "mp"), None), P(("mp", "dp"), None)),
        check_vma=False,
    )
```
